32 devices in a mesh: section: 2 (over y), ep: 16 (over z, x, core).
Axes of the slice: x: 2, y: 2, z: 4, core: 2. Of those that a mesh axis runs over, the one named last changes fastest.
Arguments:
- inputs: bfloat16 [2, 2048, 1536], P('section', 'ep'), may hold values from -6 to 6
- upstream: bfloat16 [2, 2048, 1536], P('section', 'ep'), may hold values from -6 to 6
- gate_saved: bfloat16 [2, 2048, 8, 384], P('section', 'ep'), may hold values from -6 to 6
- expert_ids: int32 [2, 2048, 8], P('section', 'ep'), may hold values from 0 to 31, all different within a row; in each aligned block of 128 rows (0 to 127, 128 to 255, ..., all dimensions but the last counted through in order) at most 48 rows name the same one
- route_weights: float32 [2, 2048, 8], P('section', 'ep'), may hold values from 0.05 to 0.5
- w_up: bfloat16 [2, 32, 1536, 384], P('section', 'ep'), may hold values from -0.15625 to 0.15625
- w_down: bfloat16 [2, 32, 384, 1536], P('section', 'ep'), may hold values from -0.3125 to 0.3125
Outputs:
- delivered: bfloat16 [2, 2048, 1536], P('section', 'ep')
- grad_up: bfloat16 [2, 32, 1536, 384], P('section', 'ep')
- grad_down: bfloat16 [2, 32, 384, 1536], P('section', 'ep')
The draws below stay inside these ranges and needn't reach their ends.
Inputs may be any that keep to these rules, and one draw needn't show every extreme that they name: `expert_ids`: each row names 8 different experts. In the rows of one device no expert is named more than 48 times, and in every draw some expert is named exactly 48 times in the rows of some device; every expert is named somewhere.
All inputs are finite; a program needn't handle non-finite values.
Results may differ from the reference program's by a relative error of at most 0.012.
Values may be sent and summed in bfloat16 or wider, within the bound.
A program may use at most 192 MiB of HBM per device.

```python
import math
import jax
import jax.numpy as jnp
import numpy as np
from jax import lax

D = 1536
FF = 384
TOP = 8
TOK_DEV = 128
EXPERTS = 32
TOKENS = 2048
CAP = 48
N_SECTION = 2
N_EP = 16


def level_of(stream_key, shape, split, least, high):
    loudness, own = 1.0, jax.random.fold_in(stream_key, 6)
    for dim, parts in split:
        heights = jnp.exp(jax.random.uniform(jax.random.fold_in(own, dim), (parts,), jnp.float32, least / len(split), high / len(split)))
        loudness = loudness * jnp.repeat(heights, shape[dim] // parts).reshape([-1 if axis == dim else 1 for axis in range(len(shape))])
    return loudness


def assign_block(key, own, number, rows, amount, top, most, skew):
    order = jax.random.permutation(key, amount)
    packed, common = load_shares(amount, rows * top, most, skew, True), load_shares(amount, rows * top, most, skew, False)
    places = jnp.arange(amount)

    def named(sizes, rotation):
        used = int((sizes > 0).sum())
        fixed = max(1, used // 4)
        shifted = fixed + (places - fixed + rotation * (used - fixed)) % max(1, amount - fixed)
        return jnp.zeros((amount,), jnp.int32).at[order[jnp.where(places < fixed, places, shifted)]].set(jnp.asarray(sizes, jnp.int32))

    sizes = jnp.where(number % 4 == 0, named(packed, number // 4), named(common, number - number // 4 - 1))
    mixed = jax.random.permutation(jax.random.fold_in(own, 3), amount)
    donor, taker = mixed[0:amount // 2 * 2:2], mixed[1:amount // 2 * 2:2]
    slack = jnp.minimum(sizes[donor] - 1, most - sizes[taker]) // 2
    slack = jnp.where((donor == order[0]) | (taker == order[0]) | (sizes[taker] == 0), 0, jnp.maximum(slack, 0))
    shifted = jax.random.randint(jax.random.fold_in(own, 4), (amount // 2,), 0, 1 << 20) % (slack + 1)
    sizes = sizes.at[donor].add(-shifted).at[taker].add(shifted)
    labels = jnp.searchsorted(jnp.cumsum(sizes), jnp.arange(rows * top), side="right").astype(jnp.int32)
    table = labels.reshape(top, rows).T
    table = table[jax.random.permutation(jax.random.fold_in(own, 1), rows)]
    rotation = jax.random.randint(jax.random.fold_in(own, 2), (rows, 1), 0, top)
    return jnp.take_along_axis(table, (jnp.arange(top)[None, :] + rotation) % top, axis=1)


def load_shares(amount, total, most, slope, full):
    portions = [(1 << 20) // math.isqrt(rank ** slope) + 1 for rank in range(1, amount + 1)]
    largest = most if full else min(most, max(-(-total // amount), total * portions[0] // sum(portions)))
    least = 1 if total - largest >= amount - 1 else 0
    holding, surplus = [largest] + [least] * (amount - 1), total - largest - least * (amount - 1)
    while surplus > 0:
        free = [i for i in range(1, amount) if holding[i] < largest] or [i for i in range(1, amount) if holding[i] < most]
        whole, left = sum([portions[i] for i in free]), surplus
        for i in free:
            extra = min(most - holding[i], max(1, left * portions[i] // whole), surplus)
            holding[i] = holding[i] + extra
            surplus = surplus - extra
    return np.array(holding)


def gaussian(key, dims, deviation, limit, cuts=(), kind=jnp.bfloat16):
    result = jax.random.normal(key, dims, jnp.float32) * deviation
    if len(cuts) > 0:
        result = level_of(key, dims, cuts, -0.22, 0.18) * result
    return jnp.clip(result, min=-limit, max=limit).astype(kind)


def setup_inputs(seed: int = 0) -> dict:
    arg_keys = jax.random.split(jax.random.key(seed), 8)
    inputs = gaussian(arg_keys[0], (N_SECTION, TOKENS, D), 1.0, 6.0, ((0, 2), (1, 16)))
    upstream = gaussian(arg_keys[1], (N_SECTION, TOKENS, D), 1.0, 6.0, ((0, 2), (1, 16)))
    gate_saved = gaussian(arg_keys[2], (N_SECTION, TOKENS, TOP, FF), 1.5, 6.0, ((0, 2), (1, 16)))
    expert_ids_keys = jax.random.split(jax.random.fold_in(arg_keys[3], 1), N_SECTION * TOKENS // TOK_DEV)
    expert_ids_turns = jax.random.permutation(jax.random.fold_in(arg_keys[3], 3), N_SECTION * TOKENS // TOK_DEV)
    expert_ids = jax.vmap(lambda own, number: assign_block(jax.random.fold_in(arg_keys[3], 2), own, number, TOK_DEV, EXPERTS, TOP, CAP, 2))(expert_ids_keys, expert_ids_turns).reshape((N_SECTION, TOKENS, TOP))
    route_weights = jnp.clip(jnp.exp(math.log(0.5) - 2.3025851 * jax.random.uniform(arg_keys[4], (N_SECTION, TOKENS, TOP), jnp.float32) ** level_of(arg_keys[4], (N_SECTION, TOKENS, TOP), ((0, 2), (1, 16)), -0.2, 0.2)), 0.05, 0.5)
    w_up = gaussian(arg_keys[5], (N_SECTION, EXPERTS, D, FF), D ** -0.5, 0.15625, ((0, 2), (1, 16)))
    w_down = gaussian(arg_keys[6], (N_SECTION, EXPERTS, FF, D), FF ** -0.5, 0.3125, ((0, 2), (1, 16)))
    return {"inputs": inputs, "upstream": upstream, "gate_saved": gate_saved, "expert_ids": expert_ids, "route_weights": route_weights, "w_up": w_up, "w_down": w_down}


def one_section(operands):
    tokens_here, cotangent, gate_layer, id_layer, weight_layer, up_layer, down_layer = operands
    rows_block = TOK_DEV * TOP
    flat_ids = id_layer.reshape(N_EP, rows_block)
    onehot = (flat_ids[:, :, None] == jnp.arange(EXPERTS, dtype=jnp.int32)[None, None, :]).astype(jnp.int32)
    position = jnp.sum(jnp.cumsum(onehot, axis=1) * onehot, axis=2) - 1
    sources = jnp.arange(N_EP, dtype=jnp.int32)[:, None]
    slot_index = (sources * CAP + position).astype(jnp.int32)
    flat_index = jnp.arange(N_EP * rows_block, dtype=jnp.int32).reshape(N_EP, rows_block)
    table = jnp.full((EXPERTS, N_EP * CAP), N_EP * rows_block, jnp.int32)
    table = table.at[flat_ids, slot_index].set(flat_index)
    gate_flat = gate_layer.reshape(TOKENS * TOP, FF)
    weight_flat = weight_layer.reshape(TOKENS * TOP)

    def per_expert(carry, expert_args):
        slot_rows, up_weight, down_weight = expert_args
        token_of = (slot_rows // TOP).astype(jnp.int32)
        x_rows = jnp.take(tokens_here, token_of, axis=0, mode="fill", fill_value=0)
        gate_rows = jnp.take(gate_flat, slot_rows, axis=0, mode="fill", fill_value=0)
        scale_rows = jnp.take(weight_flat, slot_rows, axis=0, mode="fill", fill_value=0)
        cot_rows = jnp.take(cotangent, token_of, axis=0, mode="fill", fill_value=0)
        scaled = (scale_rows[:, None] * cot_rows.astype(jnp.float32)).astype(jnp.bfloat16)
        activation = jax.nn.silu(gate_rows.astype(jnp.float32))
        up_value = jnp.dot(x_rows, up_weight, preferred_element_type=jnp.float32)
        hidden = (activation * up_value).astype(jnp.bfloat16)
        grad_down = jnp.dot(hidden.T, scaled, preferred_element_type=jnp.float32)
        grad_hidden = jnp.dot(scaled, down_weight.T, preferred_element_type=jnp.float32)
        grad_rows = (grad_hidden * activation).astype(jnp.bfloat16)
        grad_up = jnp.dot(x_rows.T, grad_rows, preferred_element_type=jnp.float32)
        slot_grad = jnp.dot(grad_rows, up_weight.T, preferred_element_type=jnp.float32).astype(jnp.bfloat16)
        carry = carry.at[token_of].add(slot_grad.astype(jnp.float32), mode="drop")
        return carry, (grad_up.astype(jnp.bfloat16), grad_down.astype(jnp.bfloat16))

    start = jnp.zeros((TOKENS, D), jnp.float32)
    layer_grad, grads = lax.scan(per_expert, start, (table, up_layer, down_layer))
    return layer_grad.astype(jnp.bfloat16), grads[0], grads[1]


def reference(inputs, upstream, gate_saved, expert_ids, route_weights, w_up, w_down):
    cot_all = jnp.roll(upstream, -1, axis=0)
    layer_grads, grad_up, grad_down = lax.map(one_section, (inputs, cot_all, gate_saved, expert_ids, route_weights, w_up, w_down))
    delivered = jnp.roll(layer_grads, -1, axis=0)
    return delivered, grad_up, grad_down
```

```python
import functools

import jax
import jax.numpy as jnp
from jax import lax
from jax.experimental import pallas as pl
from jax.experimental.pallas import tpu as pltpu
from jax.sharding import PartitionSpec as P

BF16 = jnp.bfloat16
F32 = jnp.float32
MESH = pl.DeviceIdType.MESH
VMEM_BYTES = 67_000_000
TN = (((0,), (0,)), ((), ()))
NT = (((1,), (1,)), ((), ()))


def dot(a, b, dims=(((1,), (0,)), ((), ()))):
    return lax.dot_general(a, b, dims, preferred_element_type=F32)


def iota(shape, dim):
    return lax.broadcasted_iota(jnp.int32, shape, dim)


def kernel(
    ns, ep, toks, top, width, ff, local, cap,
    x_in, up_in, gate_in, wup_in, wdn_in, idr_ref, wr_ref, idt_ref,
    out_ref, gup_ref, gdn_ref,
    xc, pay, paysend, idt, gate, act, slots, wup, wdn, dense, hid, grd, part,
    own, sibsend, sibrecv, rss, rsr, fin, gtile, dtile,
    ring_s, ring_r, sib_s, sib_r, pay_s, pay_r, id_s, id_r, ps_s, ps_r, rs_s, rs_r,
    y_s, y_r, loc, gsem, dsem,
):
    n = ep // 2
    half = n // 2
    sec = lax.axis_index("section")
    me = lax.axis_index("ep")
    core = lax.rem(me, 2)
    chip = lax.div(me, 2)
    sib = me + 1 - 2 * core
    a, b = lax.div(chip, 2), lax.rem(chip, 2)
    pos = (1 - b) * a + b * (n - 1 - a)
    w2 = width // 2
    lff = local * ff
    lcap = local * cap
    two = 2 * toks

    def chip_at(q):
        h = lax.div(q, half)
        return (1 - h) * (2 * q) + h * (2 * (n - 1 - q) + 1)

    def rows(dev):
        return pl.ds(pl.multiple_of(dev * toks, toks), toks)

    def here(dev):
        return (sec, dev)

    def remote(src, dst, s, r, to):
        return pltpu.make_async_remote_copy(
            src_ref=src, dst_ref=dst, send_sem=s, recv_sem=r, device_id=to, device_id_type=MESH
        )

    nxt = [chip_at(lax.rem(pos + 1, n)) * 2 + core, chip_at(lax.rem(pos + n - 1, n)) * 2 + core]
    sec_to = lax.rem(sec + ns - 1, ns)
    sec_from = lax.rem(sec + 1, ns)

    bar = pltpu.get_barrier_semaphore()
    greet = [(sec_to, me)] + ([(sec_from, me)] if ns > 2 else [])

    def hello(i, _):
        pl.semaphore_signal(bar, inc=1, device_id=here(lax.rem(me + i, ep)), device_id_type=MESH)
        return 0

    for to in greet:
        pl.semaphore_signal(bar, inc=1, device_id=to, device_id_type=MESH)
    lax.fori_loop(1, ep, hello, 0)

    local_copies = [
        pltpu.make_async_copy(x_in, xc.at[0, rows(me)], loc.at[0]),
        pltpu.make_async_copy(gate_in, gate, loc.at[1]),
        pltpu.make_async_copy(wdn_in, wdn, loc.at[2]),
    ] + [
        pltpu.make_async_copy(wup_in.at[e], wup.at[:, pl.ds(e * ff, ff)], loc.at[3 + e]) for e in range(local)
    ]
    for c in local_copies:
        c.start()
    pl.semaphore_wait(bar, ep - 1 + len(greet))

    def ridx(d, s, piece):
        return (d * (half + 1) + s) * 2 + piece

    def ring(src, piece, dev, d, s):
        i = ridx(d, s, piece)
        return remote(src, xc.at[piece, rows(dev)], ring_s.at[i], ring_r.at[i], here(nxt[d]))

    def side(src, piece, dev, r):
        i = r * 2 + piece
        return remote(src, xc.at[piece, rows(dev)], sib_s.at[i], sib_r.at[i], here(sib))

    cot = remote(up_in, xc.at[1, rows(me)], y_s.at[0], y_r.at[0], (sec_to, me))
    cot.start()
    for d in (0, 1):
        ring(x_in, 0, me, d, 1).start()
    side(x_in, 0, me, 0).start()
    idt[me] = idt_ref[...]

    def tell(i, _):
        to = lax.rem(me + i, ep)
        remote(idt_ref, idt.at[me], id_s.at[i], id_r.at[me], here(to)).start()
        return 0

    lax.fori_loop(1, ep, tell, 0)

    experts = ep * local
    lanes = idr_ref.shape[1]
    tri = (iota((lanes, lanes), 0) < iota((lanes, lanes), 1)).astype(BF16)
    base = jnp.zeros((experts, 1), F32)
    for k in range(idr_ref.shape[0]):
        ids = idr_ref[k : k + 1, :]
        hot = (iota((experts, lanes), 0).astype(F32) == ids).astype(F32)
        cum = dot(hot.astype(BF16), tri) + base
        base = base + jnp.sum(hot, axis=1, keepdims=True)
        slots[k : k + 1, :] = ids * cap + jnp.sum(hot * cum, axis=0, keepdims=True)

    local_copies[1].wait()

    def silu_rows(k, _):
        r = pl.ds(pl.multiple_of(k * lanes, lanes), lanes)
        v = gate[r, :].astype(F32)
        act[r, :] = (v / (1.0 + jnp.exp(-v))).astype(BF16)
        return 0

    lax.fori_loop(0, idr_ref.shape[0], silu_rows, 0)
    group = 4 * lcap

    def pack(m, _):
        acc = jnp.zeros((group, ff), F32)
        at = (iota((group, lanes), 0) + m * group).astype(F32)
        for k in range(idr_ref.shape[0]):
            pick = jnp.where(at == slots[k : k + 1, :], wr_ref[k : k + 1, :], 0.0).astype(BF16)
            acc = acc + dot(pick, act[k * lanes : (k + 1) * lanes, :])
        for j in range(4):
            paysend[m * 4 + j] = acc[j * lcap : (j + 1) * lcap].astype(BF16)
        return 0

    lax.fori_loop(0, ep // 4, pack, 0)

    def give(i, _):
        to = lax.rem(me + i, ep)
        remote(paysend.at[to], pay.at[me], pay_s.at[i], pay_r.at[me], here(to)).start()
        return 0

    lax.fori_loop(1, ep, give, 0)
    pay[me] = paysend[me]

    cot.wait_recv()
    for d in (0, 1):
        ring(xc.at[1, rows(me)], 1, me, d, 1).start()
    side(xc.at[1, rows(me)], 1, me, 0).start()
    for c in [local_copies[0]] + local_copies[2:]:
        c.wait()

    upper = (iota((toks, toks), 0) < iota((toks, toks), 1)).astype(BF16)

    def arrive(piece, dev, d, s):
        ring(xc.at[piece, rows(dev)], piece, dev, d, s).wait_recv()

    def chunk(r):
        q = chip_at(lax.rem(pos + r, n))
        other = q * 2 + 1 - core
        for piece in (0, 1):
            side(xc.at[piece, rows(other)], piece, other, r).wait_recv()
        for j in (0, 1):
            src = q * 2 + j

            @pl.when(src != me)
            def _():
                remote(paysend.at[src], pay.at[src], pay_s.at[0], pay_r.at[src], here(src)).wait_recv()
                remote(idt_ref, idt.at[src], id_s.at[0], id_r.at[src], here(src)).wait_recv()

            names = idt[src]
            for e in range(local):
                mine = (me * local + e).astype(F32)
                member = jnp.sum((names == mine).astype(F32), axis=0, keepdims=True)
                rank = dot(jnp.broadcast_to(member, (8, toks)).astype(BF16), upper)[0:1, :]
                key = jnp.where(member > 0.0, rank, -1.0)
                spread = (iota((cap, toks), 0).astype(F32) == key).astype(BF16)
                dense[j * toks : (j + 1) * toks, e * ff : (e + 1) * ff] = dot(
                    spread, pay[src, e * cap : (e + 1) * cap, :], TN
                )
        both = pl.ds(pl.multiple_of(q * two, two), two)
        u = dot(xc[0, both, :], wup[...])
        hid[both, :] = (dense[...] * u).astype(BF16)
        h = dot(xc[1, both, :], wdn[...], NT)
        g = (dense[...] * h).astype(BF16)
        grd[both, :] = g
        part[...] = dot(g, wup[...], NT)
        sibsend[r] = part[pl.ds(pl.multiple_of((1 - core) * toks, toks), toks), :].astype(BF16)
        remote(sibsend.at[r], sibrecv.at[r], ps_s.at[r], ps_r.at[r], here(sib)).start()
        own[r] = part[pl.ds(pl.multiple_of(core * toks, toks), toks), :]

    def event(it, _):
        s = lax.div(it, 2) + 1
        piece = lax.rem(it, 2)

        @pl.when(it < 2 * (half - 1))
        def _():
            for d in (0, 1):
                r = (n - s) if d == 0 else s
                dev = chip_at(lax.rem(pos + r, n)) * 2 + core
                arrive(piece, dev, d, s)
                src = xc.at[piece, rows(dev)]

                @pl.when((s + 1 < half) | (piece == d))
                def _():
                    ring(src, piece, dev, d, s + 1).start()

                side(src, piece, dev, r).start()

        @pl.when(it == 2 * half)
        def _():
            for d in (0, 1):
                dev = chip_at(lax.rem(pos + half, n)) * 2 + core
                arrive(d, dev, d, half)
                side(xc.at[d, rows(dev)], d, dev, half).start()

        @pl.when(it != 1)
        def _():
            dist = lax.div(it, 2)
            chunk((1 - piece) * dist + piece * (n - dist))

        return 0

    lax.fori_loop(0, 2 * half + 1, event, 0)

    cols = [slice(0, w2), slice(w2, width)]

    def xsum(d, t, c):
        i = (d * (half + 1) + t) * 2 + c
        return remote(
            rss.at[d, t - 1, :, cols[c]], rsr.at[d, t - 1, :, cols[c]], rs_s.at[i], rs_r.at[i], here(nxt[d])
        )

    def sib_part(r):
        remote(sibsend.at[r], sibrecv.at[r], ps_s.at[r], ps_r.at[r], here(sib)).wait_recv()

    def base_sum(r, c):
        return own[r, :, cols[c]] + sibrecv[r, :, cols[c]].astype(F32)

    def up_copy(i, slot):
        return [
            pltpu.make_async_copy(
                gtile.at[slot, e], gup_ref.at[e, pl.ds(i * 256, 256), :], gsem.at[slot * local + e]
            )
            for e in range(local)
        ]

    def up_tile(i, _):
        slot = lax.rem(i, 2)
        col = pl.ds(pl.multiple_of(i * 256, 256), 256)

        @pl.when(i >= 2)
        def _():
            for c in up_copy(i, slot):
                c.wait()

        res = dot(xc[0, :, col], grd[...], TN)
        for e in range(local):
            gtile[slot, e] = res[:, e * ff : (e + 1) * ff].astype(BF16)
        for c in up_copy(i, slot):
            c.start()
        return 0

    def down_copy(i, slot):
        return pltpu.make_async_copy(dtile.at[slot], gdn_ref.at[pl.ds(i * 256, 256), :], dsem.at[slot])

    def down_tile(i, _):
        slot = lax.rem(i, 2)
        col = pl.ds(pl.multiple_of(i * 256, 256), 256)

        @pl.when(i >= 2)
        def _():
            down_copy(i, slot).wait()

        dtile[slot] = dot(hid[:, col], xc[1], TN).astype(BF16)
        down_copy(i, slot).start()
        return 0

    n_up, n_down = width // 256, lff // 256
    tiles = n_up + n_down

    def filler(t):
        lo, hi = tiles * t // half, tiles * (t + 1) // half
        if lo < min(hi, n_up):
            lax.fori_loop(lo, min(hi, n_up), up_tile, 0)
        if max(lo, n_up) < hi:
            lax.fori_loop(max(lo, n_up) - n_up, hi - n_up, down_tile, 0)

    for t in range(half):
        dist = half - t
        rel = [dist, n - dist]
        if t == 0:
            sib_part(half)
            for d in (0, 1):
                rss[d, 0, :, cols[d]] = base_sum(half, d).astype(BF16)
                xsum(d, 1, d).start()
        else:
            for d in (0, 1):
                sib_part(rel[d])
            for step in (0, 1):
                for d in (0, 1):
                    c = (1 - d) if step == 0 else d
                    total = base_sum(rel[d], c)
                    if t > 1 or c == d:
                        xsum(d, t, c).wait_recv()
                        total = total + rsr[d, t - 1, :, cols[c]].astype(F32)
                    rss[d, t, :, cols[c]] = total.astype(BF16)
                    xsum(d, t + 1, c).start()
        filler(t)
    sib_part(0)
    done = []
    for c in (0, 1):
        for d in (0, 1):
            xsum(d, half, c).wait_recv()
        total = base_sum(0, c) + rsr[0, half - 1, :, cols[c]].astype(F32) + rsr[1, half - 1, :, cols[c]].astype(F32)
        fin[:, cols[c]] = total.astype(BF16)
        last = remote(
            fin.at[:, cols[c]], out_ref.at[:, cols[c]], y_s.at[1 + c], y_r.at[1 + c], (sec_to, me)
        )
        last.start()
        done.append(last)

    cot.wait_send()
    for d in (0, 1):
        for s in range(1, half + 1):
            for piece in (0, 1):
                if s < half or piece == d:
                    ring(xc.at[piece, rows(me)], piece, me, d, s).wait_send()
    for r in range(n):
        for piece in (0, 1):
            side(xc.at[piece, rows(me)], piece, me, r).wait_send()
        remote(sibsend.at[r], sibrecv.at[r], ps_s.at[r], ps_r.at[r], here(sib)).wait_send()

    def told(i, _):
        to = lax.rem(me + i, ep)
        remote(idt_ref, idt.at[me], id_s.at[i], id_r.at[me], here(to)).wait_send()
        remote(paysend.at[to], pay.at[me], pay_s.at[i], pay_r.at[me], here(to)).wait_send()
        return 0

    lax.fori_loop(1, ep, told, 0)
    for d in (0, 1):
        for t in range(half):
            for c in (0, 1):
                if t > 0 or c == d:
                    xsum(d, t + 1, c).wait_send()
    for slot in range(min(2, n_up)):
        for c in up_copy(slot, slot):
            c.wait()
    for slot in range(min(2, n_down)):
        down_copy(slot, slot).wait()
    for c in done:
        c.wait()


def fused_body(ns, ep, inputs, upstream, gate_saved, expert_ids, route_weights, w_up, w_down):
    toks, top = expert_ids.shape[1:]
    local, width, ff = w_up.shape[1:]
    experts = local * ep
    cap = 3 * toks * top // (2 * experts)
    n, half = ep // 2, ep // 4
    lff, lcap = local * ff, local * cap
    flat = toks * top
    lanes = 256
    ids = expert_ids[0].astype(F32)
    idr = ids.reshape(flat // lanes, lanes)
    wr = route_weights[0].reshape(flat // lanes, lanes)
    idt = ids.T
    hbm = pl.BlockSpec(memory_space=pl.ANY)
    vmem = pl.BlockSpec(memory_space=pltpu.VMEM)
    dma = pltpu.SemaphoreType.DMA
    out, gup, gdn = pl.pallas_call(
        functools.partial(kernel, ns, ep, toks, top, width, ff, local, cap),
        out_shape=(
            jax.ShapeDtypeStruct((toks, width), BF16),
            jax.ShapeDtypeStruct((local, width, ff), BF16),
            jax.ShapeDtypeStruct((lff, width), BF16),
        ),
        in_specs=[hbm] * 5 + [vmem] * 3,
        out_specs=(hbm, hbm, hbm),
        scratch_shapes=[
            pltpu.VMEM((2, ep * toks, width), BF16),
            pltpu.VMEM((ep, lcap, ff), BF16),
            pltpu.VMEM((ep, lcap, ff), BF16),
            pltpu.VMEM((ep, top, toks), F32),
            pltpu.VMEM((flat, ff), BF16),
            pltpu.VMEM((flat, ff), BF16),
            pltpu.VMEM((flat // lanes, lanes), F32),
            pltpu.VMEM((width, lff), BF16),
            pltpu.VMEM((lff, width), BF16),
            pltpu.VMEM((2 * toks, lff), F32),
            pltpu.VMEM((ep * toks, lff), BF16),
            pltpu.VMEM((ep * toks, lff), BF16),
            pltpu.VMEM((2 * toks, width), F32),
            pltpu.VMEM((n, toks, width), F32),
            pltpu.VMEM((n, toks, width), BF16),
            pltpu.VMEM((n, toks, width), BF16),
            pltpu.VMEM((2, half, toks, width), BF16),
            pltpu.VMEM((2, half, toks, width), BF16),
            pltpu.VMEM((toks, width), BF16),
            pltpu.VMEM((2, local, 256, ff), BF16),
            pltpu.VMEM((2, 256, width), BF16),
            dma((4 * (half + 1),)),
            dma((4 * (half + 1),)),
            dma((2 * n,)),
            dma((2 * n,)),
            dma((ep,)),
            dma((ep,)),
            dma((ep,)),
            dma((ep,)),
            dma((n,)),
            dma((n,)),
            dma((4 * (half + 1),)),
            dma((4 * (half + 1),)),
            dma((3,)),
            dma((3,)),
            dma((3 + local,)),
            dma((2 * local,)),
            dma((2,)),
        ],
        compiler_params=pltpu.CompilerParams(
            collective_id=0, has_side_effects=True, vmem_limit_bytes=VMEM_BYTES
        ),
    )(
        inputs[0], upstream[0], gate_saved[0].reshape(flat, ff), w_up[0],
        w_down[0].reshape(lff, width), idr, wr, idt,
    )
    return out[None], gup[None], gdn.reshape(1, local, ff, width)


def from_behind(block, axis, distance):
    devices = range(lax.axis_size(axis))
    route = [((i - distance) % len(devices), i) for i in devices]
    return lax.ppermute(block, axis, route)


def plain_body(inputs, upstream, gate_saved, expert_ids, route_weights, w_up, w_down):
    ep = lax.axis_size("ep")
    local = w_up.shape[1]
    experts = local * ep
    toks, top = expert_ids.shape[1:]
    cap = 3 * toks * top // (2 * experts)
    width = inputs.shape[2]
    ff = w_up.shape[3]

    routing = jnp.concatenate([expert_ids[0].astype(F32), route_weights[0]], axis=1)
    routing_all = lax.all_gather(routing, "ep", axis=0, tiled=False)

    ids = expert_ids[0]
    hit = ids[:, :, None] == jnp.arange(experts, dtype=jnp.int32)
    member = jnp.any(hit, axis=1).astype(BF16)
    lower = (jnp.arange(toks)[:, None] > jnp.arange(toks)[None, :]).astype(BF16)
    rank = jnp.dot(lower, member, preferred_element_type=F32)
    place = jnp.sum(jnp.where(hit, rank[:, None, :], 0.0), axis=2)
    slot = (ids * cap + place.astype(jnp.int32)).reshape(1, toks * top)
    pick = (jnp.arange(experts * cap, dtype=jnp.int32)[:, None] == slot).astype(BF16)
    gate_send = jnp.dot(pick, gate_saved[0].reshape(toks * top, ff), preferred_element_type=F32)
    gate_send = gate_send.astype(BF16).reshape(ep, local, cap, ff)
    gate_recv = lax.all_to_all(gate_send, "ep", split_axis=0, concat_axis=0, tiled=True)

    cot = from_behind(upstream, "section", -1)[0]
    x_all = lax.all_gather(inputs[0], "ep", axis=0, tiled=True)
    c_all = lax.all_gather(cot, "ep", axis=0, tiled=True)

    me = lax.axis_index("ep")
    mine = (me * local + jnp.arange(local)).astype(F32)
    hits = routing_all[:, :, :top, None] == mine
    weight = jnp.sum(jnp.where(hits, routing_all[:, :, top:, None], 0.0), axis=2)
    members = jnp.any(hits, axis=2)
    ranks = jnp.einsum("ab,sbe->sae", lower, members.astype(BF16), preferred_element_type=F32)
    ranks = jnp.where(members, ranks, -1.0)
    spread = (ranks[:, :, :, None] == jnp.arange(cap).astype(F32)).astype(BF16)
    gate = jnp.einsum("stec,secf->stef", spread, gate_recv, preferred_element_type=F32)
    act = jax.nn.silu(gate).reshape(ep * toks, local, ff)
    act_w = (act * weight.reshape(ep * toks, local, 1)).reshape(ep * toks, local * ff)

    up_cat = jnp.transpose(w_up[0], (1, 0, 2)).reshape(width, local * ff)
    down_cat = w_down[0].reshape(local * ff, width)
    u = jnp.dot(x_all, up_cat, preferred_element_type=F32)
    hidden = (act_w * u).astype(BF16)
    h = dot(c_all, down_cat, NT)
    g = (act_w * h).astype(BF16)
    part = dot(g, up_cat, NT)
    grad = lax.psum_scatter(part.astype(BF16), "ep", scatter_dimension=0, tiled=True)
    delivered = from_behind(grad[None], "section", -1)
    grad_down = dot(hidden, c_all, TN)
    grad_up = jnp.stack([dot(x_all, g[:, e * ff : (e + 1) * ff], TN) for e in range(local)])
    return (
        delivered,
        grad_up.astype(BF16)[None],
        grad_down.astype(BF16).reshape(1, local, ff, width),
    )


def solution(mesh):
    ns, ep = mesh.shape["section"], mesh.shape["ep"]

    def body(*args):
        toks, width = args[0].shape[1:]
        local, ff = args[5].shape[1], args[5].shape[3]
        rows = ep * toks
        need = rows * (4 * width + 4 * local * ff) + 12 * rows * width // 2 + 4 * local * ff * width
        if need < 0.75 * VMEM_BYTES and ep % 4 == 0:
            return fused_body(ns, ep, *args)
        return plain_body(*args)

    return jax.shard_map(
        body,
        mesh=mesh,
        in_specs=(
            P("section", "ep", None),
            P("section", "ep", None),
            P("section", "ep", None, None),
            P("section", "ep", None),
            P("section", "ep", None),
            P("section", "ep", None, None),
            P("section", "ep", None, None),
        ),
        out_specs=(
            P("section", "ep", None),
            P("section", "ep", None, None),
            P("section", "ep", None, None),
        ),
        check_vma=False,
    )
```

```python
import functools

import jax
import jax.numpy as jnp
from jax import lax
from jax.experimental import pallas as pl
from jax.experimental.pallas import tpu as pltpu
from jax.sharding import PartitionSpec as P

BF16 = jnp.bfloat16
F32 = jnp.float32
MESH = pl.DeviceIdType.MESH
VMEM_BYTES = 58_000_000
TN = (((0,), (0,)), ((), ()))
NT = (((1,), (1,)), ((), ()))


def dot(a, b, dims=(((1,), (0,)), ((), ()))):
    return lax.dot_general(a, b, dims, preferred_element_type=F32)


def iota(shape, dim):
    return lax.broadcasted_iota(jnp.int32, shape, dim)


def kernel(
    ns, ep, toks, top, width, ff, local, cap,
    x_in, up_in, gate_in, wup_in, wdn_in, idt_ref, wt_ref,
    out_ref, gup_ref, gdn_ref,
    xc, pay, paysend, idt, gate, act, slots, wflat, wup, wdn, dense, hid, grd, part,
    own, sibsend, sibrecv, rss, rsr, fin, finr,
    ring_s, ring_r, col_s, row_s, cot_r, sib_s, sib_r, pay_s, pay_r, id_s, id_r, ps_s, ps_r, rs_s, rs_r,
    y_s, y_r, loc,
):
    n = ep // 2
    half = n // 2
    sec = lax.axis_index("section")
    me = lax.axis_index("ep")
    core = lax.rem(me, 2)
    chip = lax.div(me, 2)
    sib = me + 1 - 2 * core
    a, b = lax.div(chip, 2), lax.rem(chip, 2)
    pos = (1 - b) * a + b * (n - 1 - a)
    w2, w4 = width // 2, width // 4
    cols = [slice(0, w2), slice(w2, width)]
    quarters = [slice(c * w4, (c + 1) * w4) for c in range(4)]
    lff = local * ff
    lcap = local * cap
    two = 2 * toks

    def chip_at(q):
        h = lax.div(q, half)
        return (1 - h) * (2 * q) + h * (2 * (n - 1 - q) + 1)

    def rows(dev):
        return pl.ds(pl.multiple_of(dev * toks, toks), toks)

    def here(dev):
        return (sec, dev)

    def remote(src, dst, s, r, to):
        return pltpu.make_async_remote_copy(
            src_ref=src, dst_ref=dst, send_sem=s, recv_sem=r, device_id=to, device_id_type=MESH
        )

    nxt = [chip_at(lax.rem(pos + 1, n)) * 2 + core, chip_at(lax.rem(pos + n - 1, n)) * 2 + core]
    sec_to = lax.rem(sec + ns - 1, ns)
    sec_from = lax.rem(sec + 1, ns)

    bar = pltpu.get_barrier_semaphore()
    across = [me] + nxt
    greet = [(sec_to, dev) for dev in across] + ([(sec_from, dev) for dev in across] if ns > 2 else [])

    def hello(i, _):
        pl.semaphore_signal(bar, inc=1, device_id=here(lax.rem(me + i, ep)), device_id_type=MESH)
        return 0

    for to in greet:
        pl.semaphore_signal(bar, inc=1, device_id=to, device_id_type=MESH)
    lax.fori_loop(1, ep, hello, 0)

    local_copies = [
        pltpu.make_async_copy(x_in, xc.at[0, rows(me)], loc.at[0]),
        pltpu.make_async_copy(gate_in, gate, loc.at[1]),
        pltpu.make_async_copy(wdn_in, wdn, loc.at[2]),
    ] + [
        pltpu.make_async_copy(wup_in.at[e], wup.at[:, pl.ds(e * ff, ff)], loc.at[3 + e]) for e in range(local)
    ]
    for c in local_copies:
        c.start()
    pl.semaphore_wait(bar, ep - 1 + len(greet))

    def ring(src, dev, d, s):
        i = d * (half + 1) + s
        return remote(src, xc.at[0, rows(dev)], ring_s.at[i], ring_r.at[i], here(nxt[d]))

    def ring_last(dev, d):
        ref = xc.at[0, rows(dev), cols[d]]
        i = d * (half + 1) + half
        return remote(ref, ref, ring_s.at[i], ring_r.at[i], here(nxt[d]))

    def side(src, piece, q, dev):
        i = q * 2 + piece
        return remote(src, xc.at[piece, rows(dev)], sib_s.at[i], sib_r.at[i], here(sib))

    def column(owner, s, d):
        ref = xc.at[1, rows((owner * 2 + b) * 2 + core)]
        to = ((a + 1 - 2 * d) * 2 + b) * 2 + core
        return remote(ref, ref, col_s.at[d * half + s], cot_r.at[owner * 2 + b], here(to))

    def row(owner):
        ref = xc.at[1, rows((owner * 2 + b) * 2 + core)]
        to = (a * 2 + 1 - b) * 2 + core
        return remote(ref, ref, row_s.at[owner], cot_r.at[owner * 2 + b], here(to))

    def cot_arrive(q):
        ref = xc.at[1, rows(q * 2 + core)]
        remote(ref, ref, row_s.at[0], cot_r.at[q], here(sib)).wait_recv()

    def cot_side(q):
        return side(xc.at[1, rows(q * 2 + core)], 1, q, q * 2 + core)

    cot = remote(up_in, xc.at[1, rows(me)], y_s.at[0], y_r.at[0], (sec_to, me))
    cot.start()
    for d in (0, 1):
        ring(x_in, me, d, 1).start()
    side(x_in, 0, chip, me).start()
    idt[me] = idt_ref[...]

    def tell(i, _):
        to = lax.rem(me + i, ep)
        remote(idt_ref, idt.at[me], id_s.at[i], id_r.at[me], here(to)).start()
        return 0

    lax.fori_loop(1, ep, tell, 0)

    experts = ep * local
    lanes = 256
    parts = toks * top // lanes
    span = lanes // top
    tri = (iota((lanes, lanes), 0) < iota((lanes, lanes), 1)).astype(BF16)
    base = jnp.zeros((experts, 1), F32)
    ids_t = idt_ref[...].astype(F32).astype(BF16)
    w_t = wt_ref[...].astype(BF16)
    mine_k = iota((top, lanes), 0) == lax.rem(iota((top, lanes), 1), top)
    for k in range(parts):
        token = lax.div(iota((toks, lanes), 1), top) + k * span
        take = (iota((toks, lanes), 0) == token).astype(BF16)
        ids = jnp.sum(jnp.where(mine_k, dot(ids_t, take), 0.0), axis=0, keepdims=True)
        wflat[k : k + 1, :] = jnp.sum(jnp.where(mine_k, dot(w_t, take), 0.0), axis=0, keepdims=True)
        hot = (iota((experts, lanes), 0).astype(F32) == ids).astype(F32)
        cum = dot(hot.astype(BF16), tri) + base
        base = base + jnp.sum(hot, axis=1, keepdims=True)
        slots[k : k + 1, :] = ids * cap + jnp.sum(hot * cum, axis=0, keepdims=True)

    local_copies[1].wait()

    def silu_rows(k, _):
        r = pl.ds(pl.multiple_of(k * lanes, lanes), lanes)
        v = gate[r, :].astype(F32)
        act[r, :] = (v / (1.0 + jnp.exp(-v))).astype(BF16)
        return 0

    lax.fori_loop(0, parts, silu_rows, 0)
    group = 4 * lcap

    def pack(m, _):
        acc = jnp.zeros((group, ff), F32)
        at = (iota((group, lanes), 0) + m * group).astype(F32)
        for k in range(parts):
            pick = jnp.where(at == slots[k : k + 1, :], wflat[k : k + 1, :], 0.0).astype(BF16)
            acc = acc + dot(pick, act[k * lanes : (k + 1) * lanes, :])
        for j in range(4):
            paysend[m * 4 + j] = acc[j * lcap : (j + 1) * lcap].astype(BF16)
        return 0

    lax.fori_loop(0, ep // 4, pack, 0)

    def give(i, _):
        to = lax.rem(me + i, ep)
        remote(paysend.at[to], pay.at[me], pay_s.at[i], pay_r.at[me], here(to)).start()
        return 0

    lax.fori_loop(1, ep, give, 0)
    pay[me] = paysend[me]

    def reaches(d):
        return (a + 1 < half) if d == 0 else (a >= 1)

    cot.wait_recv()
    for d in (0, 1):

        @pl.when(reaches(d))
        def _():
            column(a, 0, d).start()

    row(a).start()
    cot_side(chip).start()
    for c in [local_copies[0]] + local_copies[2:]:
        c.wait()

    upper = (iota((toks, toks), 0) < iota((toks, toks), 1)).astype(BF16)

    def chunk(r):
        q = chip_at(lax.rem(pos + r, n))
        other = q * 2 + 1 - core
        for piece in (0, 1):
            side(xc.at[piece, rows(other)], piece, q, other).wait_recv()
        for j in (0, 1):
            src = q * 2 + j

            @pl.when(src != me)
            def _():
                remote(paysend.at[src], pay.at[src], pay_s.at[0], pay_r.at[src], here(src)).wait_recv()
                remote(idt_ref, idt.at[src], id_s.at[0], id_r.at[src], here(src)).wait_recv()

            names = idt[src]
            for e in range(local):
                member = jnp.sum((names == me * local + e).astype(F32), axis=0, keepdims=True)
                rank = dot(jnp.broadcast_to(member, (8, toks)).astype(BF16), upper)[0:1, :]
                key = jnp.where(member > 0.0, rank, -1.0)
                spread = (iota((cap, toks), 0).astype(F32) == key).astype(BF16)
                dense[j * toks : (j + 1) * toks, e * ff : (e + 1) * ff] = dot(
                    spread, pay[src, e * cap : (e + 1) * cap, :], TN
                )
        both = pl.ds(pl.multiple_of(q * two, two), two)
        u = dot(xc[0, both, :], wup[...])
        hid[both, :] = (dense[...] * u).astype(BF16)
        h = dot(xc[1, both, :], wdn[...], NT)
        g = (dense[...] * h).astype(BF16)
        grd[both, :] = g
        part[...] = dot(g, wup[...], NT)
        sibsend[r] = part[pl.ds(pl.multiple_of((1 - core) * toks, toks), toks), :].astype(BF16)
        remote(sibsend.at[r], sibrecv.at[r], ps_s.at[r], ps_r.at[r], here(sib)).start()
        own[r] = part[pl.ds(pl.multiple_of(core * toks, toks), toks), :]

    def hop(d, t, c):
        i = (d * (half + 1) + t) * 4 + c
        ref = quarters[c]
        to = (sec_to, nxt[d]) if t == half else here(nxt[d])
        return remote(rss.at[d, t - 1, :, ref], rsr.at[d, t - 1, :, ref], rs_s.at[i], rs_r.at[i], to)

    def sib_part(r):
        remote(sibsend.at[r], sibrecv.at[r], ps_s.at[r], ps_r.at[r], here(sib)).wait_recv()

    def send_sum(t, side_of, first):
        for j in (0, 1):
            for d in (0, 1):
                c = 2 * (d if side_of == 0 else 1 - d) + j
                r = (half - t) if d == 0 else n - (half - t)
                total = own[r, :, quarters[c]] + sibrecv[r, :, quarters[c]].astype(F32)
                if not first:
                    hop(d, t, c).wait_recv()
                    total = total + rsr[d, t - 1, :, quarters[c]].astype(F32)
                rss[d, t, :, quarters[c]] = total.astype(BF16)
                hop(d, t + 1, c).start()

    def early(t):
        for d in (0, 1):
            sib_part((half - t) if d == 0 else n - (half - t))
        send_sum(t, 1, t == 1)

    own_part = remote(fin, finr, y_s.at[1], y_r.at[1], (sec_to, me))

    last = 2 * half - 2

    def event(it, _):
        s = lax.div(it, 2) + 1
        turn = lax.rem(it, 2)

        @pl.when((it < last) & (turn == 0))
        def _():
            for d in (0, 1):
                q = chip_at(lax.rem(pos + ((n - s) if d == 0 else s), n))
                dev = q * 2 + core
                src = xc.at[0, rows(dev)]
                ring(src, dev, d, s).wait_recv()

                @pl.when(s + 1 < half)
                def _():
                    ring(src, dev, d, s + 1).start()

                @pl.when(s + 1 == half)
                def _():
                    ring_last(dev, d).start()

                side(src, 0, q, dev).start()

        def from_row(owner):
            @pl.when((owner >= 0) & (owner < half))
            def _():
                q = owner * 2 + 1 - b
                cot_arrive(q)
                cot_side(q).start()

        @pl.when((it < last) & (turn == 1))
        def _():
            for d in (0, 1):
                owner = a - s + 2 * s * d

                @pl.when((owner >= 0) & (owner < half))
                def _():
                    q = owner * 2 + b
                    cot_arrive(q)

                    @pl.when(reaches(d))
                    def _():
                        column(owner, s, d).start()

                    row(owner).start()
                    cot_side(q).start()

            from_row(a + s - 1)

            @pl.when(s > 1)
            def _():
                from_row(a - s + 1)

        @pl.when(it == 2)
        def _():
            sib_part(0)
            fin[...] = (own[0] + sibrecv[0].astype(F32)).astype(BF16)
            own_part.start()

        @pl.when(it == last)
        def _():
            early(1)
            q = chip_at(lax.rem(pos + half, n))
            dev = q * 2 + core
            for d in (0, 1):
                ring_last(dev, d).wait_recv()
            side(xc.at[0, rows(dev)], 0, q, dev).start()
            from_row(a + half - 1)
            from_row(a - half + 1)

        away = s * jnp.minimum(it, 1)

        def compute(j, _):
            chunk(away + j * (n - 2 * away))
            return 0

        ends = (it == 0).astype(jnp.int32) + (it == last).astype(jnp.int32)
        lax.fori_loop(0, 2 * turn + ends, compute, 0)
        return 0

    lax.fori_loop(0, last + 1, event, 0)

    def up_tile(i, _):
        col = pl.ds(pl.multiple_of(i * 256, 256), 256)
        res = dot(xc[0, :, col], grd[...], TN)
        for e in range(local):
            gup_ref[e, col, :] = res[:, e * ff : (e + 1) * ff].astype(BF16)
        return 0

    def down_tile(i, _):
        col = pl.ds(pl.multiple_of(i * 256, 256), 256)
        gdn_ref[col, :] = dot(hid[:, col], xc[1], TN).astype(BF16)
        return 0

    n_up, n_down = width // 256, lff // 256
    tiles = n_up + n_down

    def filler(t):
        lo, hi = tiles * t // half, tiles * (t + 1) // half
        if lo < min(hi, n_up):
            lax.fori_loop(lo, min(hi, n_up), up_tile, 0)
        if max(lo, n_up) < hi:
            lax.fori_loop(max(lo, n_up) - n_up, hi - n_up, down_tile, 0)

    sib_part(half)
    for t in range(half):
        send_sum(t, 0, t == 0)
        filler(t)
        if t + 2 < half:
            early(t + 2)
    own_part.wait_recv()
    for part_of in (1, 0):
        for j in (0, 1):
            for d in (0, 1):
                c = 2 * (d if part_of == 0 else 1 - d) + j
                hop(d, half, c).wait_recv()
                got = rsr[d, half - 1, :, quarters[c]].astype(F32)
                if part_of == 1:
                    own[0, :, quarters[c]] = finr[:, quarters[c]].astype(F32) + got
                else:
                    out_ref[:, quarters[c]] = (own[0, :, quarters[c]] + got).astype(BF16)

    cot.wait_send()
    own_part.wait_send()
    for d in (0, 1):
        for s in range(1, half):
            ring(xc.at[0, rows(me)], me, d, s).wait_send()
        ring_last(me, d).wait_send()
        for s in range(half):
            owner = a - s + 2 * s * d

            @pl.when(reaches(d) & (owner >= 0) & (owner < half))
            def _():
                column(owner, s, d).wait_send()

    for owner in range(half):
        row(owner).wait_send()
    for r in range(n):
        for piece in (0, 1):
            side(xc.at[piece, rows(me)], piece, r, me).wait_send()
        remote(sibsend.at[r], sibrecv.at[r], ps_s.at[r], ps_r.at[r], here(sib)).wait_send()

    def told(i, _):
        to = lax.rem(me + i, ep)
        remote(idt_ref, idt.at[me], id_s.at[i], id_r.at[me], here(to)).wait_send()
        remote(paysend.at[to], pay.at[me], pay_s.at[i], pay_r.at[me], here(to)).wait_send()
        return 0

    lax.fori_loop(1, ep, told, 0)
    for d in (0, 1):
        for t in range(half):
            for c in range(4):
                if t > 0 or c // 2 == d:
                    hop(d, t + 1, c).wait_send()


def fused_body(ns, ep, inputs, upstream, gate_saved, expert_ids, route_weights, w_up, w_down):
    toks, top = expert_ids.shape[1:]
    local, width, ff = w_up.shape[1:]
    experts = local * ep
    cap = 3 * toks * top // (2 * experts)
    n, half = ep // 2, ep // 4
    lff, lcap = local * ff, local * cap
    flat = toks * top
    hbm = pl.BlockSpec(memory_space=pl.ANY)
    vmem = pl.BlockSpec(memory_space=pltpu.VMEM)
    dma = pltpu.SemaphoreType.DMA
    out, gup, gdn = pl.pallas_call(
        functools.partial(kernel, ns, ep, toks, top, width, ff, local, cap),
        out_shape=(
            pltpu.VMEM((toks, width), BF16),
            pltpu.VMEM((local, width, ff), BF16),
            pltpu.VMEM((lff, width), BF16),
        ),
        in_specs=[hbm] * 5 + [vmem] * 2,
        out_specs=(vmem, vmem, vmem),
        scratch_shapes=[
            pltpu.VMEM((2, ep * toks, width), BF16),
            pltpu.VMEM((ep, lcap, ff), BF16),
            pltpu.VMEM((ep, lcap, ff), BF16),
            pltpu.VMEM((ep, top, toks), jnp.int32),
            pltpu.VMEM((flat, ff), BF16),
            pltpu.VMEM((flat, ff), BF16),
            pltpu.VMEM((flat // 256, 256), F32),
            pltpu.VMEM((flat // 256, 256), F32),
            pltpu.VMEM((width, lff), BF16),
            pltpu.VMEM((lff, width), BF16),
            pltpu.VMEM((2 * toks, lff), F32),
            pltpu.VMEM((ep * toks, lff), BF16),
            pltpu.VMEM((ep * toks, lff), BF16),
            pltpu.VMEM((2 * toks, width), F32),
            pltpu.VMEM((n, toks, width), F32),
            pltpu.VMEM((n, toks, width), BF16),
            pltpu.VMEM((n, toks, width), BF16),
            pltpu.VMEM((2, half, toks, width), BF16),
            pltpu.VMEM((2, half, toks, width), BF16),
            pltpu.VMEM((toks, width), BF16),
            pltpu.VMEM((toks, width), BF16),
            dma((2 * (half + 1),)),
            dma((2 * (half + 1),)),
            dma((2 * half,)),
            dma((half,)),
            dma((n,)),
            dma((2 * n,)),
            dma((2 * n,)),
            dma((ep,)),
            dma((ep,)),
            dma((ep,)),
            dma((ep,)),
            dma((n,)),
            dma((n,)),
            dma((8 * (half + 1),)),
            dma((8 * (half + 1),)),
            dma((2,)),
            dma((2,)),
            dma((3 + local,)),
        ],
        compiler_params=pltpu.CompilerParams(
            collective_id=0, has_side_effects=True, vmem_limit_bytes=VMEM_BYTES
        ),
    )(
        inputs[0], upstream[0], gate_saved[0].reshape(flat, ff), w_up[0],
        w_down[0].reshape(lff, width), expert_ids[0].T, route_weights[0].T,
    )
    return out[None], gup[None], gdn.reshape(1, local, ff, width)


def from_behind(block, axis, distance):
    devices = range(lax.axis_size(axis))
    route = [((i - distance) % len(devices), i) for i in devices]
    return lax.ppermute(block, axis, route)


def plain_body(inputs, upstream, gate_saved, expert_ids, route_weights, w_up, w_down):
    ep = lax.axis_size("ep")
    local = w_up.shape[1]
    experts = local * ep
    toks, top = expert_ids.shape[1:]
    cap = 3 * toks * top // (2 * experts)
    width = inputs.shape[2]
    ff = w_up.shape[3]

    routing = jnp.concatenate([expert_ids[0].astype(F32), route_weights[0]], axis=1)
    routing_all = lax.all_gather(routing, "ep", axis=0, tiled=False)

    ids = expert_ids[0]
    hit = ids[:, :, None] == jnp.arange(experts, dtype=jnp.int32)
    member = jnp.any(hit, axis=1).astype(BF16)
    lower = (jnp.arange(toks)[:, None] > jnp.arange(toks)[None, :]).astype(BF16)
    rank = jnp.dot(lower, member, preferred_element_type=F32)
    place = jnp.sum(jnp.where(hit, rank[:, None, :], 0.0), axis=2)
    slot = (ids * cap + place.astype(jnp.int32)).reshape(1, toks * top)
    pick = (jnp.arange(experts * cap, dtype=jnp.int32)[:, None] == slot).astype(BF16)
    gate_send = jnp.dot(pick, gate_saved[0].reshape(toks * top, ff), preferred_element_type=F32)
    gate_send = gate_send.astype(BF16).reshape(ep, local, cap, ff)
    gate_recv = lax.all_to_all(gate_send, "ep", split_axis=0, concat_axis=0, tiled=True)

    cot = from_behind(upstream, "section", -1)[0]
    x_all = lax.all_gather(inputs[0], "ep", axis=0, tiled=True)
    c_all = lax.all_gather(cot, "ep", axis=0, tiled=True)

    me = lax.axis_index("ep")
    mine = (me * local + jnp.arange(local)).astype(F32)
    hits = routing_all[:, :, :top, None] == mine
    weight = jnp.sum(jnp.where(hits, routing_all[:, :, top:, None], 0.0), axis=2)
    members = jnp.any(hits, axis=2)
    ranks = jnp.einsum("ab,sbe->sae", lower, members.astype(BF16), preferred_element_type=F32)
    ranks = jnp.where(members, ranks, -1.0)
    spread = (ranks[:, :, :, None] == jnp.arange(cap).astype(F32)).astype(BF16)
    gate = jnp.einsum("stec,secf->stef", spread, gate_recv, preferred_element_type=F32)
    act = jax.nn.silu(gate).reshape(ep * toks, local, ff)
    act_w = (act * weight.reshape(ep * toks, local, 1)).reshape(ep * toks, local * ff)

    up_cat = jnp.transpose(w_up[0], (1, 0, 2)).reshape(width, local * ff)
    down_cat = w_down[0].reshape(local * ff, width)
    u = jnp.dot(x_all, up_cat, preferred_element_type=F32)
    hidden = (act_w * u).astype(BF16)
    h = dot(c_all, down_cat, NT)
    g = (act_w * h).astype(BF16)
    part = dot(g, up_cat, NT)
    grad = lax.psum_scatter(part.astype(BF16), "ep", scatter_dimension=0, tiled=True)
    delivered = from_behind(grad[None], "section", -1)
    grad_down = dot(hidden, c_all, TN)
    grad_up = jnp.stack([dot(x_all, g[:, e * ff : (e + 1) * ff], TN) for e in range(local)])
    return (
        delivered,
        grad_up.astype(BF16)[None],
        grad_down.astype(BF16).reshape(1, local, ff, width),
    )


def solution(mesh):
    ns, ep = mesh.shape["section"], mesh.shape["ep"]

    def body(*args):
        toks, width = args[0].shape[1:]
        local, ff = args[5].shape[1], args[5].shape[3]
        rows = ep * toks
        need = rows * (4 * width + 4 * local * ff) + 12 * rows * width // 2 + 4 * local * ff * width
        if need < 0.75 * VMEM_BYTES and ep % 8 == 0:
            return fused_body(ns, ep, *args)
        return plain_body(*args)

    return jax.shard_map(
        body,
        mesh=mesh,
        in_specs=(
            P("section", "ep", None),
            P("section", "ep", None),
            P("section", "ep", None, None),
            P("section", "ep", None),
            P("section", "ep", None),
            P("section", "ep", None, None),
            P("section", "ep", None, None),
        ),
        out_specs=(
            P("section", "ep", None),
            P("section", "ep", None, None),
            P("section", "ep", None, None),
        ),
        check_vma=False,
    )
```

```python
import functools

import jax
import jax.numpy as jnp
from jax import lax
from jax.experimental import pallas as pl
from jax.experimental.pallas import tpu as pltpu
from jax.sharding import PartitionSpec as P

BF16 = jnp.bfloat16
F32 = jnp.float32
MESH = pl.DeviceIdType.MESH
VMEM_BYTES = 58_000_000
TN = (((0,), (0,)), ((), ()))
NT = (((1,), (1,)), ((), ()))


def dot(a, b, dims=(((1,), (0,)), ((), ()))):
    return lax.dot_general(a, b, dims, preferred_element_type=F32)


def iota(shape, dim):
    return lax.broadcasted_iota(jnp.int32, shape, dim)


def kernel(
    ns, ep, toks, top, width, ff, local, cap,
    x_in, up_in, gate_in, wup_in, wdn_in, idt_ref, wt_ref,
    out_ref, gup_ref, gdn_ref,
    xc, pay, paysend, idt, gate, act, slots, wflat, wup, wdn, hid, grd, part,
    own, sibsend, sibrecv, rss, rsr, fin, finr, over,
    ring_s, ring_r, col_s, row_s, cot_r, sib_s, sib_r, pay_s, pay_r, id_s, id_r, ps_s, ps_r, rs_s, rs_r,
    y_s, y_r, over_s, over_r, loc,
):
    n = ep // 2
    half = n // 2
    sec = lax.axis_index("section")
    me = lax.axis_index("ep")
    core = lax.rem(me, 2)
    chip = lax.div(me, 2)
    sib = me + 1 - 2 * core
    a, b = lax.div(chip, 2), lax.rem(chip, 2)
    pos = (1 - b) * a + b * (n - 1 - a)
    w2, w4 = width // 2, width // 4
    cols = [slice(0, w2), slice(w2, width)]
    quarters = [slice(c * w4, (c + 1) * w4) for c in range(4)]
    lff = local * ff
    lcap = local * cap
    two = 2 * toks

    def chip_at(q):
        h = lax.div(q, half)
        return (1 - h) * (2 * q) + h * (2 * (n - 1 - q) + 1)

    def rows(dev):
        return pl.ds(pl.multiple_of(dev * toks, toks), toks)

    def here(dev):
        return (sec, dev)

    def remote(src, dst, s, r, to):
        return pltpu.make_async_remote_copy(
            src_ref=src, dst_ref=dst, send_sem=s, recv_sem=r, device_id=to, device_id_type=MESH
        )

    nxt = [chip_at(lax.rem(pos + 1, n)) * 2 + core, chip_at(lax.rem(pos + n - 1, n)) * 2 + core]
    sec_to = lax.rem(sec + ns - 1, ns)
    sec_from = lax.rem(sec + 1, ns)

    bar = pltpu.get_barrier_semaphore()
    across = [me]
    greet = [(sec_to, dev) for dev in across] + ([(sec_from, dev) for dev in across] if ns > 2 else [])

    def hello(i, _):
        pl.semaphore_signal(bar, inc=1, device_id=here(lax.rem(me + i, ep)), device_id_type=MESH)
        return 0

    for to in greet:
        pl.semaphore_signal(bar, inc=1, device_id=to, device_id_type=MESH)
    lax.fori_loop(1, ep, hello, 0)

    local_copies = [
        pltpu.make_async_copy(x_in, xc.at[0, rows(me)], loc.at[0]),
        pltpu.make_async_copy(gate_in, gate, loc.at[1]),
        pltpu.make_async_copy(wdn_in, wdn, loc.at[2]),
    ] + [
        pltpu.make_async_copy(wup_in.at[e], wup.at[:, pl.ds(e * ff, ff)], loc.at[3 + e]) for e in range(local)
    ]
    for c in local_copies:
        c.start()
    pl.semaphore_wait(bar, ep - 1 + len(greet))

    def ring(src, dev, d, s):
        i = d * (half + 1) + s
        return remote(src, xc.at[0, rows(dev)], ring_s.at[i], ring_r.at[i], here(nxt[d]))

    def ring_last(dev, d):
        ref = xc.at[0, rows(dev), cols[d]]
        i = d * (half + 1) + half
        return remote(ref, ref, ring_s.at[i], ring_r.at[i], here(nxt[d]))

    def side(src, piece, q, dev):
        i = q * 2 + piece
        return remote(src, xc.at[piece, rows(dev)], sib_s.at[i], sib_r.at[i], here(sib))

    def column(owner, s, d):
        ref = xc.at[1, rows((owner * 2 + b) * 2 + core)]
        to = ((a + 1 - 2 * d) * 2 + b) * 2 + core
        return remote(ref, ref, col_s.at[d * half + s], cot_r.at[owner * 2 + b], here(to))

    def row(owner):
        ref = xc.at[1, rows((owner * 2 + b) * 2 + core)]
        to = (a * 2 + 1 - b) * 2 + core
        return remote(ref, ref, row_s.at[owner], cot_r.at[owner * 2 + b], here(to))

    def cot_arrive(q):
        ref = xc.at[1, rows(q * 2 + core)]
        remote(ref, ref, row_s.at[0], cot_r.at[q], here(sib)).wait_recv()

    def cot_side(q):
        return side(xc.at[1, rows(q * 2 + core)], 1, q, q * 2 + core)

    cot = remote(up_in, xc.at[1, rows(me)], y_s.at[0], y_r.at[0], (sec_to, me))
    cot.start()
    for d in (0, 1):
        ring(x_in, me, d, 1).start()
    side(x_in, 0, chip, me).start()
    idt[me] = idt_ref[...]

    def tell(i, _):
        to = lax.rem(me + i, ep)
        remote(idt_ref, idt.at[me], id_s.at[i], id_r.at[me], here(to)).start()
        return 0

    lax.fori_loop(1, ep, tell, 0)

    experts = ep * local
    lanes = 256
    parts = toks * top // lanes
    span = lanes // top
    tri = (iota((lanes, lanes), 0) < iota((lanes, lanes), 1)).astype(BF16)
    base = jnp.zeros((experts, 1), F32)
    ids_t = idt_ref[...].astype(F32).astype(BF16)
    w_t = wt_ref[...].astype(BF16)
    mine_k = iota((top, lanes), 0) == lax.rem(iota((top, lanes), 1), top)
    for k in range(parts):
        token = lax.div(iota((toks, lanes), 1), top) + k * span
        take = (iota((toks, lanes), 0) == token).astype(BF16)
        ids = jnp.sum(jnp.where(mine_k, dot(ids_t, take), 0.0), axis=0, keepdims=True)
        wflat[k : k + 1, :] = jnp.sum(jnp.where(mine_k, dot(w_t, take), 0.0), axis=0, keepdims=True)
        hot = (iota((experts, lanes), 0).astype(F32) == ids).astype(F32)
        cum = dot(hot.astype(BF16), tri) + base
        base = base + jnp.sum(hot, axis=1, keepdims=True)
        slots[k : k + 1, :] = ids * cap + jnp.sum(hot * cum, axis=0, keepdims=True)

    local_copies[1].wait()

    def silu_rows(k, _):
        r = pl.ds(pl.multiple_of(k * lanes, lanes), lanes)
        v = gate[r, :].astype(F32)
        act[r, :] = (v / (1.0 + jnp.exp(-v))).astype(BF16)
        return 0

    lax.fori_loop(0, parts, silu_rows, 0)
    group = 4 * lcap

    def pack(m, _):
        acc = jnp.zeros((group, ff), F32)
        at = (iota((group, lanes), 0) + m * group).astype(F32)
        for k in range(parts):
            pick = jnp.where(at == slots[k : k + 1, :], wflat[k : k + 1, :], 0.0).astype(BF16)
            acc = acc + dot(pick, act[k * lanes : (k + 1) * lanes, :])
        for j in range(4):
            paysend[m * 4 + j] = acc[j * lcap : (j + 1) * lcap].astype(BF16)
        return 0

    lax.fori_loop(0, ep // 4, pack, 0)

    def give(i, _):
        to = lax.rem(me + i, ep)
        remote(paysend.at[to], pay.at[me], pay_s.at[i], pay_r.at[me], here(to)).start()
        return 0

    lax.fori_loop(1, ep, give, 0)
    pay[me] = paysend[me]

    def reaches(d):
        return (a + 1 < half) if d == 0 else (a >= 1)

    cot.wait_recv()
    for d in (0, 1):

        @pl.when(reaches(d))
        def _():
            column(a, 0, d).start()

    row(a).start()
    cot_side(chip).start()
    for c in [local_copies[0]] + local_copies[2:]:
        c.wait()

    upper = (iota((toks, toks), 0) < iota((toks, toks), 1)).astype(BF16)

    def chunk_of(k):
        odd = lax.rem(k, 2)
        r = odd * lax.div(k + 1, 2) + (1 - odd) * lax.rem(n - lax.div(k, 2), n)
        q = chip_at(lax.rem(pos + r, n))
        return r, q, pl.ds(pl.multiple_of(q * two, two), two)

    def other_side(piece, q):
        dev = q * 2 + 1 - core
        side(xc.at[piece, rows(dev)], piece, q, dev).wait_recv()

    def spread(k, _):
        r, q, both = chunk_of(k)
        for j in (0, 1):
            src = q * 2 + j

            @pl.when(src != me)
            def _():
                remote(paysend.at[src], pay.at[src], pay_s.at[0], pay_r.at[src], here(src)).wait_recv()
                remote(idt_ref, idt.at[src], id_s.at[0], id_r.at[src], here(src)).wait_recv()

            names = idt[src]
            for e in range(local):
                member = jnp.sum((names == me * local + e).astype(F32), axis=0, keepdims=True)
                rank = dot(jnp.broadcast_to(member, (8, toks)).astype(BF16), upper)[0:1, :]
                key = jnp.where(member > 0.0, rank, -1.0)
                to_slot = (iota((cap, toks), 0).astype(F32) == key).astype(BF16)
                grd[rows(src), e * ff : (e + 1) * ff] = dot(
                    to_slot, pay[src, e * cap : (e + 1) * cap, :], TN
                ).astype(BF16)
        return 0

    def stage_x(k, _):
        r, q, both = chunk_of(k)
        other_side(0, q)
        hid[both, :] = (grd[both, :].astype(F32) * dot(xc[0, both, :], wup[...])).astype(BF16)
        return 0

    def stage_c(k, _):
        r, q, both = chunk_of(k)
        other_side(1, q)
        g = (grd[both, :].astype(F32) * dot(xc[1, both, :], wdn[...], NT)).astype(BF16)
        grd[both, :] = g
        part[...] = dot(g, wup[...], NT)
        sibsend[r] = part[pl.ds(pl.multiple_of((1 - core) * toks, toks), toks), :].astype(BF16)
        remote(sibsend.at[r], sibrecv.at[r], ps_s.at[r], ps_r.at[r], here(sib)).start()
        own[r] = part[pl.ds(pl.multiple_of(core * toks, toks), toks), :]
        return 0

    def hop(d, t, c):
        i = (d * (half + 1) + t) * 4 + c
        ref = quarters[c]
        src = over.at[d, :, ref] if t == half else rss.at[d, t - 1, :, ref]
        return remote(src, rsr.at[d, t - 1, :, ref], rs_s.at[i], rs_r.at[i], here(nxt[d]))

    def cross(d, c):
        i = d * 4 + c
        ref = quarters[c]
        return remote(rss.at[d, half - 1, :, ref], over.at[d, :, ref], over_s.at[i], over_r.at[i], (sec_to, me))

    def quarters_of(side_of):
        return [(d, 2 * (d if side_of == 0 else 1 - d) + j) for j in (0, 1) for d in (0, 1)]

    def pass_on(side_of):
        for d, c in quarters_of(side_of):
            cross(d, c).wait_recv()
            hop(d, half, c).start()

    def sib_part(r):
        remote(sibsend.at[r], sibrecv.at[r], ps_s.at[r], ps_r.at[r], here(sib)).wait_recv()

    def send_sum(t, side_of, first, ways=(0, 1)):
        for d, c in [p for p in quarters_of(side_of) if p[0] in ways]:
            r = (half - t) if d == 0 else n - (half - t)
            total = own[r, :, quarters[c]] + sibrecv[r, :, quarters[c]].astype(F32)
            if not first:
                hop(d, t, c).wait_recv()
                total = total + rsr[d, t - 1, :, quarters[c]].astype(F32)
            rss[d, t, :, quarters[c]] = total.astype(BF16)
            if t + 1 < half:
                hop(d, t + 1, c).start()
            else:
                cross(d, c).start()

    def early(t):
        for d in (0, 1):
            sib_part((half - t) if d == 0 else n - (half - t))
            if t == 1:
                send_sum(t, 1, True, (d,))
        if t > 1:
            send_sum(t, 1, False)

    own_part = remote(fin, finr, y_s.at[1], y_r.at[1], (sec_to, me))

    last = 2 * half - 2

    def event(it, _):
        s = lax.div(it, 2) + 1
        turn = lax.rem(it, 2)

        @pl.when((it < last) & (turn == 0))
        def _():
            for d in (0, 1):
                q = chip_at(lax.rem(pos + ((n - s) if d == 0 else s), n))
                dev = q * 2 + core
                src = xc.at[0, rows(dev)]
                ring(src, dev, d, s).wait_recv()

                @pl.when(s + 1 < half)
                def _():
                    ring(src, dev, d, s + 1).start()

                @pl.when(s + 1 == half)
                def _():
                    ring_last(dev, d).start()

                side(src, 0, q, dev).start()

        def from_row(owner):
            @pl.when((owner >= 0) & (owner < half))
            def _():
                q = owner * 2 + 1 - b
                cot_arrive(q)
                cot_side(q).start()

        @pl.when((it < last) & (turn == 1))
        def _():
            for d in (0, 1):
                owner = a - s + 2 * s * d

                @pl.when((owner >= 0) & (owner < half))
                def _():
                    q = owner * 2 + b
                    cot_arrive(q)

                    @pl.when(reaches(d))
                    def _():
                        column(owner, s, d).start()

                    row(owner).start()
                    cot_side(q).start()

            from_row(a + s - 1)

            @pl.when(s > 1)
            def _():
                from_row(a - s + 1)

        @pl.when(it == 2)
        def _():
            sib_part(0)
            fin[...] = (own[0] + sibrecv[0].astype(F32)).astype(BF16)
            own_part.start()

        @pl.when(it == last)
        def _():
            q = chip_at(lax.rem(pos + half, n))
            dev = q * 2 + core
            for d in (0, 1):
                ring_last(dev, d).wait_recv()
            side(xc.at[0, rows(dev)], 0, q, dev).start()
            early(1)
            from_row(a + half - 1)
            from_row(a - half + 1)

        final = (it == last).astype(jnp.int32)
        x_lo = (it + jnp.minimum(it, 1)) * (1 - final) + (n - 1) * final
        x_hi = x_lo + (1 - turn) * ((2 + (it == 0).astype(jnp.int32)) * (1 - final) + final)
        ahead = (1 - turn) * (1 - final) * (x_hi - x_lo + (it == last - 2).astype(jnp.int32))
        lax.fori_loop(x_lo, x_lo + ahead, spread, 0)
        lax.fori_loop(x_lo, x_hi, stage_x, 0)
        c_lo = it * (1 - final) + (n - 1) * final
        lax.fori_loop(c_lo, c_lo + 2 * turn + (it == 0).astype(jnp.int32) + final, stage_c, 0)
        return 0

    lax.fori_loop(0, last + 1, event, 0)

    def up_tile(i, _):
        col = pl.ds(pl.multiple_of(i * 256, 256), 256)
        res = dot(xc[0, :, col], grd[...], TN)
        for e in range(local):
            gup_ref[e, col, :] = res[:, e * ff : (e + 1) * ff].astype(BF16)
        return 0

    def down_tile(i, _):
        col = pl.ds(pl.multiple_of(i * 256, 256), 256)
        gdn_ref[col, :] = dot(hid[:, col], xc[1], TN).astype(BF16)
        return 0

    n_up, n_down = width // 256, lff // 256

    def fill_up(lo, hi):
        lax.fori_loop(lo, hi, up_tile, 0)

    def fill_down(lo, hi):
        lax.fori_loop(lo, hi, down_tile, 0)

    sib_part(half)
    for t in range(half):
        send_sum(t, 0, t == 0)
        if t == 1:
            fill_up(n_up // 2, n_up)
        if t + 2 < half:
            early(t + 2)
        elif t + 2 == half:
            pass_on(1)
        if t == 0:
            fill_up(0, n_up // 2)
            fill_down(0, 1)
        elif t == 1:
            fill_down(1, 2)
    fill_down(2, n_down)
    pass_on(0)
    own_part.wait_recv()
    for side_of in (1, 0):
        for d, c in quarters_of(side_of):
            hop(d, half, c).wait_recv()
            got = rsr[d, half - 1, :, quarters[c]].astype(F32)
            if side_of == 1:
                own[0, :, quarters[c]] = finr[:, quarters[c]].astype(F32) + got
            else:
                out_ref[:, quarters[c]] = (own[0, :, quarters[c]] + got).astype(BF16)

    cot.wait_send()
    own_part.wait_send()
    for d in (0, 1):
        for s in range(1, half):
            ring(xc.at[0, rows(me)], me, d, s).wait_send()
        ring_last(me, d).wait_send()
        for s in range(half):
            owner = a - s + 2 * s * d

            @pl.when(reaches(d) & (owner >= 0) & (owner < half))
            def _():
                column(owner, s, d).wait_send()

    for owner in range(half):
        row(owner).wait_send()
    for r in range(n):
        for piece in (0, 1):
            side(xc.at[piece, rows(me)], piece, r, me).wait_send()
        remote(sibsend.at[r], sibrecv.at[r], ps_s.at[r], ps_r.at[r], here(sib)).wait_send()

    def told(i, _):
        to = lax.rem(me + i, ep)
        remote(idt_ref, idt.at[me], id_s.at[i], id_r.at[me], here(to)).wait_send()
        remote(paysend.at[to], pay.at[me], pay_s.at[i], pay_r.at[me], here(to)).wait_send()
        return 0

    lax.fori_loop(1, ep, told, 0)
    for d in (0, 1):
        for t in range(half):
            for c in range(4):
                if t > 0 or c // 2 == d:
                    hop(d, t + 1, c).wait_send()
        for c in range(4):
            cross(d, c).wait_send()


def fused_body(ns, ep, inputs, upstream, gate_saved, expert_ids, route_weights, w_up, w_down):
    toks, top = expert_ids.shape[1:]
    local, width, ff = w_up.shape[1:]
    experts = local * ep
    cap = 3 * toks * top // (2 * experts)
    n, half = ep // 2, ep // 4
    lff, lcap = local * ff, local * cap
    flat = toks * top
    hbm = pl.BlockSpec(memory_space=pl.ANY)
    vmem = pl.BlockSpec(memory_space=pltpu.VMEM)
    dma = pltpu.SemaphoreType.DMA
    out, gup, gdn = pl.pallas_call(
        functools.partial(kernel, ns, ep, toks, top, width, ff, local, cap),
        out_shape=(
            pltpu.VMEM((toks, width), BF16),
            pltpu.VMEM((local, width, ff), BF16),
            pltpu.VMEM((lff, width), BF16),
        ),
        in_specs=[hbm] * 5 + [vmem] * 2,
        out_specs=(vmem, vmem, vmem),
        scratch_shapes=[
            pltpu.VMEM((2, ep * toks, width), BF16),
            pltpu.VMEM((ep, lcap, ff), BF16),
            pltpu.VMEM((ep, lcap, ff), BF16),
            pltpu.VMEM((ep, top, toks), jnp.int32),
            pltpu.VMEM((flat, ff), BF16),
            pltpu.VMEM((flat, ff), BF16),
            pltpu.VMEM((flat // 256, 256), F32),
            pltpu.VMEM((flat // 256, 256), F32),
            pltpu.VMEM((width, lff), BF16),
            pltpu.VMEM((lff, width), BF16),
            pltpu.VMEM((ep * toks, lff), BF16),
            pltpu.VMEM((ep * toks, lff), BF16),
            pltpu.VMEM((2 * toks, width), F32),
            pltpu.VMEM((n, toks, width), F32),
            pltpu.VMEM((n, toks, width), BF16),
            pltpu.VMEM((n, toks, width), BF16),
            pltpu.VMEM((2, half, toks, width), BF16),
            pltpu.VMEM((2, half, toks, width), BF16),
            pltpu.VMEM((toks, width), BF16),
            pltpu.VMEM((toks, width), BF16),
            pltpu.VMEM((2, toks, width), BF16),
            dma((2 * (half + 1),)),
            dma((2 * (half + 1),)),
            dma((2 * half,)),
            dma((half,)),
            dma((n,)),
            dma((2 * n,)),
            dma((2 * n,)),
            dma((ep,)),
            dma((ep,)),
            dma((ep,)),
            dma((ep,)),
            dma((n,)),
            dma((n,)),
            dma((8 * (half + 1),)),
            dma((8 * (half + 1),)),
            dma((2,)),
            dma((2,)),
            dma((8,)),
            dma((8,)),
            dma((3 + local,)),
        ],
        compiler_params=pltpu.CompilerParams(
            collective_id=0, has_side_effects=True, vmem_limit_bytes=VMEM_BYTES
        ),
    )(
        inputs[0], upstream[0], gate_saved[0].reshape(flat, ff), w_up[0],
        w_down[0].reshape(lff, width), expert_ids[0].T, route_weights[0].T,
    )
    return out[None], gup[None], gdn.reshape(1, local, ff, width)


def from_behind(block, axis, distance):
    devices = range(lax.axis_size(axis))
    route = [((i - distance) % len(devices), i) for i in devices]
    return lax.ppermute(block, axis, route)


def plain_body(inputs, upstream, gate_saved, expert_ids, route_weights, w_up, w_down):
    ep = lax.axis_size("ep")
    local = w_up.shape[1]
    experts = local * ep
    toks, top = expert_ids.shape[1:]
    cap = 3 * toks * top // (2 * experts)
    width = inputs.shape[2]
    ff = w_up.shape[3]

    routing = jnp.concatenate([expert_ids[0].astype(F32), route_weights[0]], axis=1)
    routing_all = lax.all_gather(routing, "ep", axis=0, tiled=False)

    ids = expert_ids[0]
    hit = ids[:, :, None] == jnp.arange(experts, dtype=jnp.int32)
    member = jnp.any(hit, axis=1).astype(BF16)
    lower = (jnp.arange(toks)[:, None] > jnp.arange(toks)[None, :]).astype(BF16)
    rank = jnp.dot(lower, member, preferred_element_type=F32)
    place = jnp.sum(jnp.where(hit, rank[:, None, :], 0.0), axis=2)
    slot = (ids * cap + place.astype(jnp.int32)).reshape(1, toks * top)
    pick = (jnp.arange(experts * cap, dtype=jnp.int32)[:, None] == slot).astype(BF16)
    gate_send = jnp.dot(pick, gate_saved[0].reshape(toks * top, ff), preferred_element_type=F32)
    gate_send = gate_send.astype(BF16).reshape(ep, local, cap, ff)
    gate_recv = lax.all_to_all(gate_send, "ep", split_axis=0, concat_axis=0, tiled=True)

    cot = from_behind(upstream, "section", -1)[0]
    x_all = lax.all_gather(inputs[0], "ep", axis=0, tiled=True)
    c_all = lax.all_gather(cot, "ep", axis=0, tiled=True)

    me = lax.axis_index("ep")
    mine = (me * local + jnp.arange(local)).astype(F32)
    hits = routing_all[:, :, :top, None] == mine
    weight = jnp.sum(jnp.where(hits, routing_all[:, :, top:, None], 0.0), axis=2)
    members = jnp.any(hits, axis=2)
    ranks = jnp.einsum("ab,sbe->sae", lower, members.astype(BF16), preferred_element_type=F32)
    ranks = jnp.where(members, ranks, -1.0)
    spread = (ranks[:, :, :, None] == jnp.arange(cap).astype(F32)).astype(BF16)
    gate = jnp.einsum("stec,secf->stef", spread, gate_recv, preferred_element_type=F32)
    act = jax.nn.silu(gate).reshape(ep * toks, local, ff)
    act_w = (act * weight.reshape(ep * toks, local, 1)).reshape(ep * toks, local * ff)

    up_cat = jnp.transpose(w_up[0], (1, 0, 2)).reshape(width, local * ff)
    down_cat = w_down[0].reshape(local * ff, width)
    u = jnp.dot(x_all, up_cat, preferred_element_type=F32)
    hidden = (act_w * u).astype(BF16)
    h = dot(c_all, down_cat, NT)
    g = (act_w * h).astype(BF16)
    part = dot(g, up_cat, NT)
    grad = lax.psum_scatter(part.astype(BF16), "ep", scatter_dimension=0, tiled=True)
    delivered = from_behind(grad[None], "section", -1)
    grad_down = dot(hidden, c_all, TN)
    grad_up = jnp.stack([dot(x_all, g[:, e * ff : (e + 1) * ff], TN) for e in range(local)])
    return (
        delivered,
        grad_up.astype(BF16)[None],
        grad_down.astype(BF16).reshape(1, local, ff, width),
    )


def solution(mesh):
    ns, ep = mesh.shape["section"], mesh.shape["ep"]

    def body(*args):
        toks, width = args[0].shape[1:]
        local, ff = args[5].shape[1], args[5].shape[3]
        rows = ep * toks
        need = rows * (4 * width + 4 * local * ff) + 12 * rows * width // 2 + 4 * local * ff * width
        if need < 0.75 * VMEM_BYTES and ep % 8 == 0:
            return fused_body(ns, ep, *args)
        return plain_body(*args)

    return jax.shard_map(
        body,
        mesh=mesh,
        in_specs=(
            P("section", "ep", None),
            P("section", "ep", None),
            P("section", "ep", None, None),
            P("section", "ep", None),
            P("section", "ep", None),
            P("section", "ep", None, None),
            P("section", "ep", None, None),
        ),
        out_specs=(
            P("section", "ep", None),
            P("section", "ep", None, None),
            P("section", "ep", None, None),
        ),
        check_vma=False,
    )
```

```python
import functools

import jax
import jax.numpy as jnp
from jax import lax
from jax.experimental import pallas as pl
from jax.experimental.pallas import tpu as pltpu
from jax.sharding import PartitionSpec as P

BF16 = jnp.bfloat16
F32 = jnp.float32
MESH = pl.DeviceIdType.MESH
VMEM_BYTES = 58_000_000
TN = (((0,), (0,)), ((), ()))
NT = (((1,), (1,)), ((), ()))


def dot(a, b, dims=(((1,), (0,)), ((), ()))):
    return lax.dot_general(a, b, dims, preferred_element_type=F32)


def iota(shape, dim):
    return lax.broadcasted_iota(jnp.int32, shape, dim)


def kernel(
    ns, ep, toks, top, width, ff, local, cap,
    x_in, up_in, gate_in, wup_in, wdn_in, idt_ref, wt_ref,
    out_ref, gup_ref, gdn_ref,
    xc, pay, paysend, idt, gate, act, slots, wflat, wup, wdn, hid, grd, part,
    own, sibsend, sibrecv, rss, rsr, fin, finr, over,
    ring_s, ring_r, col_s, row_s, cot_r, sib_s, sib_r, pay_s, pay_r, id_s, id_r, ps_s, ps_r, rs_s, rs_r,
    y_s, y_r, over_s, over_r, loc,
):
    n = ep // 2
    half = n // 2
    sec = lax.axis_index("section")
    me = lax.axis_index("ep")
    core = lax.rem(me, 2)
    chip = lax.div(me, 2)
    sib = me + 1 - 2 * core
    a, b = lax.div(chip, 2), lax.rem(chip, 2)
    pos = (1 - b) * a + b * (n - 1 - a)
    w2, w4 = width // 2, width // 4
    cols = [slice(0, w2), slice(w2, width)]
    quarters = [slice(c * w4, (c + 1) * w4) for c in range(4)]
    lff = local * ff
    lcap = local * cap
    two = 2 * toks

    def chip_at(q):
        h = lax.div(q, half)
        return (1 - h) * (2 * q) + h * (2 * (n - 1 - q) + 1)

    def rows(dev):
        return pl.ds(pl.multiple_of(dev * toks, toks), toks)

    def here(dev):
        return (sec, dev)

    def remote(src, dst, s, r, to):
        return pltpu.make_async_remote_copy(
            src_ref=src, dst_ref=dst, send_sem=s, recv_sem=r, device_id=to, device_id_type=MESH
        )

    nxt = [chip_at(lax.rem(pos + 1, n)) * 2 + core, chip_at(lax.rem(pos + n - 1, n)) * 2 + core]
    sec_to = lax.rem(sec + ns - 1, ns)
    sec_from = lax.rem(sec + 1, ns)

    bar = pltpu.get_barrier_semaphore()
    across = [me]
    greet = [(sec_to, dev) for dev in across] + ([(sec_from, dev) for dev in across] if ns > 2 else [])

    def hello(i, _):
        pl.semaphore_signal(bar, inc=1, device_id=here(lax.rem(me + i, ep)), device_id_type=MESH)
        return 0

    for to in greet:
        pl.semaphore_signal(bar, inc=1, device_id=to, device_id_type=MESH)
    lax.fori_loop(1, ep, hello, 0)

    local_copies = [
        pltpu.make_async_copy(x_in, xc.at[0, rows(me)], loc.at[0]),
        pltpu.make_async_copy(gate_in, gate, loc.at[1]),
        pltpu.make_async_copy(wdn_in, wdn, loc.at[2]),
    ] + [
        pltpu.make_async_copy(wup_in.at[e], wup.at[:, pl.ds(e * ff, ff)], loc.at[3 + e]) for e in range(local)
    ]
    for c in local_copies:
        c.start()
    pl.semaphore_wait(bar, ep - 1 + len(greet))

    def ring(src, dev, d, s):
        i = d * (half + 1) + s
        return remote(src, xc.at[0, rows(dev)], ring_s.at[i], ring_r.at[i], here(nxt[d]))

    def ring_last(dev, d):
        ref = xc.at[0, rows(dev), cols[d]]
        i = d * (half + 1) + half
        return remote(ref, ref, ring_s.at[i], ring_r.at[i], here(nxt[d]))

    def side(src, q, dev):
        return remote(src, xc.at[0, rows(dev)], sib_s.at[q * 3], sib_r.at[q * 3], here(sib))

    def cot_ref(q, h, of=core):
        return xc.at[1, rows(q * 2 + of), cols[h]]

    def column(owner, s, d, h):
        ref = cot_ref(owner * 2 + b, h)
        to = ((a + 1 - 2 * d) * 2 + b) * 2 + core
        return remote(
            ref, ref, col_s.at[(d * half + s) * 2 + h], cot_r.at[(owner * 2 + b) * 2 + h], here(to)
        )

    def row(owner, h):
        ref = cot_ref(owner * 2 + b, h)
        to = (a * 2 + 1 - b) * 2 + core
        return remote(ref, ref, row_s.at[owner * 2 + h], cot_r.at[(owner * 2 + b) * 2 + h], here(to))

    def cot_arrive(q, h):
        ref = cot_ref(q, h)
        remote(ref, ref, row_s.at[h], cot_r.at[q * 2 + h], here(sib)).wait_recv()

    def cot_side(q, h, of=core):
        ref = cot_ref(q, h, of)
        return remote(ref, ref, sib_s.at[q * 3 + 1 + h], sib_r.at[q * 3 + 1 + h], here(sib))

    def cot_in(h):
        return remote(up_in.at[:, cols[h]], cot_ref(chip, h), y_s.at[h], y_r.at[h], (sec_to, me))

    for h in (0, 1):
        cot_in(h).start()
    for d in (0, 1):
        ring(x_in, me, d, 1).start()
    side(x_in, chip, me).start()
    idt[me] = idt_ref[...]

    def tell(i, _):
        to = lax.rem(me + i, ep)
        remote(idt_ref, idt.at[me], id_s.at[i], id_r.at[me], here(to)).start()
        return 0

    lax.fori_loop(1, ep, tell, 0)

    experts = ep * local
    lanes = 256
    parts = toks * top // lanes
    span = lanes // top
    tri = (iota((lanes, lanes), 0) < iota((lanes, lanes), 1)).astype(BF16)
    base = jnp.zeros((experts, 1), F32)
    ids_t = idt_ref[...].astype(F32).astype(BF16)
    w_t = wt_ref[...].astype(BF16)
    mine_k = iota((top, lanes), 0) == lax.rem(iota((top, lanes), 1), top)
    for k in range(parts):
        token = lax.div(iota((toks, lanes), 1), top) + k * span
        take = (iota((toks, lanes), 0) == token).astype(BF16)
        ids = jnp.sum(jnp.where(mine_k, dot(ids_t, take), 0.0), axis=0, keepdims=True)
        wflat[k : k + 1, :] = jnp.sum(jnp.where(mine_k, dot(w_t, take), 0.0), axis=0, keepdims=True)
        hot = (iota((experts, lanes), 0).astype(F32) == ids).astype(F32)
        cum = dot(hot.astype(BF16), tri) + base
        base = base + jnp.sum(hot, axis=1, keepdims=True)
        slots[k : k + 1, :] = ids * cap + jnp.sum(hot * cum, axis=0, keepdims=True)

    local_copies[1].wait()

    def silu_rows(k, _):
        r = pl.ds(pl.multiple_of(k * lanes, lanes), lanes)
        v = gate[r, :].astype(F32)
        act[r, :] = (v / (1.0 + jnp.exp(-v))).astype(BF16)
        return 0

    lax.fori_loop(0, parts, silu_rows, 0)
    group = 4 * lcap

    def pack(m, _):
        acc = jnp.zeros((group, ff), F32)
        at = (iota((group, lanes), 0) + m * group).astype(F32)
        for k in range(parts):
            pick = jnp.where(at == slots[k : k + 1, :], wflat[k : k + 1, :], 0.0).astype(BF16)
            acc = acc + dot(pick, act[k * lanes : (k + 1) * lanes, :])
        for j in range(4):
            paysend[m * 4 + j] = acc[j * lcap : (j + 1) * lcap].astype(BF16)
        return 0

    lax.fori_loop(0, ep // 4, pack, 0)

    def give(i, _):
        to = lax.rem(me + i, ep)
        remote(paysend.at[to], pay.at[me], pay_s.at[i], pay_r.at[me], here(to)).start()
        return 0

    lax.fori_loop(1, ep, give, 0)
    pay[me] = paysend[me]

    def reaches(d):
        return (a + 1 < half) if d == 0 else (a >= 1)

    for h in (0, 1):
        cot_in(h).wait_recv()
        for d in (0, 1):

            @pl.when(reaches(d))
            def _():
                column(a, 0, d, h).start()

        row(a, h).start()
        cot_side(chip, h).start()
    for c in [local_copies[0]] + local_copies[2:]:
        c.wait()

    upper = (iota((toks, toks), 0) < iota((toks, toks), 1)).astype(BF16)

    def chunk_of(k):
        odd = lax.rem(k, 2)
        r = odd * lax.div(k + 1, 2) + (1 - odd) * lax.rem(n - lax.div(k, 2), n)
        q = chip_at(lax.rem(pos + r, n))
        return r, q, pl.ds(pl.multiple_of(q * two, two), two)

    def spread(k, _):
        r, q, both = chunk_of(k)
        for j in (0, 1):
            src = q * 2 + j

            @pl.when(src != me)
            def _():
                remote(paysend.at[src], pay.at[src], pay_s.at[0], pay_r.at[src], here(src)).wait_recv()
                remote(idt_ref, idt.at[src], id_s.at[0], id_r.at[src], here(src)).wait_recv()

            names = idt[src]
            for e in range(local):
                member = jnp.sum((names == me * local + e).astype(F32), axis=0, keepdims=True)
                rank = dot(jnp.broadcast_to(member, (8, toks)).astype(BF16), upper)[0:1, :]
                key = jnp.where(member > 0.0, rank, -1.0)
                to_slot = (iota((cap, toks), 0).astype(F32) == key).astype(BF16)
                grd[rows(src), e * ff : (e + 1) * ff] = dot(
                    to_slot, pay[src, e * cap : (e + 1) * cap, :], TN
                ).astype(BF16)
        return 0

    def stage_x(k, _):
        r, q, both = chunk_of(k)
        dev = q * 2 + 1 - core
        side(xc.at[0, rows(dev)], q, dev).wait_recv()
        hid[both, :] = (grd[both, :].astype(F32) * dot(xc[0, both, :], wup[...])).astype(BF16)
        return 0

    def stage_c(k, _):
        r, q, both = chunk_of(k)
        for h in (0, 1):
            cot_side(q, h, 1 - core).wait_recv()
        g = (grd[both, :].astype(F32) * dot(xc[1, both, :], wdn[...], NT)).astype(BF16)
        grd[both, :] = g
        part[...] = dot(g, wup[...], NT)
        sibsend[r] = part[pl.ds(pl.multiple_of((1 - core) * toks, toks), toks), :].astype(BF16)
        remote(sibsend.at[r], sibrecv.at[r], ps_s.at[r], ps_r.at[r], here(sib)).start()
        own[r] = part[pl.ds(pl.multiple_of(core * toks, toks), toks), :]
        return 0

    def hop(d, t, c):
        i = (d * (half + 1) + t) * 4 + c
        ref = quarters[c]
        src = over.at[d, :, ref] if t == half else rss.at[d, t - 1, :, ref]
        return remote(src, rsr.at[d, t - 1, :, ref], rs_s.at[i], rs_r.at[i], here(nxt[d]))

    def cross(d, c):
        i = d * 4 + c
        ref = quarters[c]
        return remote(rss.at[d, half - 1, :, ref], over.at[d, :, ref], over_s.at[i], over_r.at[i], (sec_to, me))

    def quarters_of(side_of):
        return [(d, 2 * (d if side_of == 0 else 1 - d) + j) for j in (0, 1) for d in (0, 1)]

    def pass_on(side_of):
        for d, c in quarters_of(side_of):
            cross(d, c).wait_recv()
            hop(d, half, c).start()

    def sib_part(r):
        remote(sibsend.at[r], sibrecv.at[r], ps_s.at[r], ps_r.at[r], here(sib)).wait_recv()

    def send_sum(t, side_of, first, ways=(0, 1)):
        for d, c in [p for p in quarters_of(side_of) if p[0] in ways]:
            r = (half - t) if d == 0 else n - (half - t)
            total = own[r, :, quarters[c]] + sibrecv[r, :, quarters[c]].astype(F32)
            if not first:
                hop(d, t, c).wait_recv()
                total = total + rsr[d, t - 1, :, quarters[c]].astype(F32)
            rss[d, t, :, quarters[c]] = total.astype(BF16)
            if t + 1 < half:
                hop(d, t + 1, c).start()
            else:
                cross(d, c).start()

    def early(t):
        for d in (0, 1):
            sib_part((half - t) if d == 0 else n - (half - t))
            if t == 1:
                send_sum(t, 1, True, (d,))
        if t > 1:
            send_sum(t, 1, False)

    own_part = remote(fin, finr, y_s.at[2], y_r.at[2], (sec_to, me))

    last = 2 * half - 2

    def event(it, _):
        s = lax.div(it, 2) + 1
        turn = lax.rem(it, 2)

        @pl.when((it < last) & (turn == 0))
        def _():
            for d in (0, 1):
                q = chip_at(lax.rem(pos + ((n - s) if d == 0 else s), n))
                dev = q * 2 + core
                src = xc.at[0, rows(dev)]
                ring(src, dev, d, s).wait_recv()

                @pl.when(s + 1 < half)
                def _():
                    ring(src, dev, d, s + 1).start()

                @pl.when(s + 1 == half)
                def _():
                    ring_last(dev, d).start()

                side(src, q, dev).start()

        def from_row(owner):
            @pl.when((owner >= 0) & (owner < half))
            def _():
                q = owner * 2 + 1 - b
                for h in (0, 1):
                    cot_arrive(q, h)
                    cot_side(q, h).start()

        @pl.when((it < last) & (turn == 1))
        def _():
            for h in (0, 1):
                for d in (0, 1):
                    owner = a - s + 2 * s * d

                    @pl.when((owner >= 0) & (owner < half))
                    def _():
                        q = owner * 2 + b
                        cot_arrive(q, h)

                        @pl.when(reaches(d))
                        def _():
                            column(owner, s, d, h).start()

                        row(owner, h).start()
                        cot_side(q, h).start()

            from_row(a + s - 1)

            @pl.when(s > 1)
            def _():
                from_row(a - s + 1)

        @pl.when(it == 2)
        def _():
            sib_part(0)
            fin[...] = (own[0] + sibrecv[0].astype(F32)).astype(BF16)
            own_part.start()

        @pl.when(it == last)
        def _():
            q = chip_at(lax.rem(pos + half, n))
            dev = q * 2 + core
            for d in (0, 1):
                ring_last(dev, d).wait_recv()
            side(xc.at[0, rows(dev)], q, dev).start()
            early(1)
            from_row(a + half - 1)
            from_row(a - half + 1)

        final = (it == last).astype(jnp.int32)
        x_lo = (it + jnp.minimum(it, 1)) * (1 - final) + (n - 1) * final
        x_hi = x_lo + (1 - turn) * ((2 + (it == 0).astype(jnp.int32)) * (1 - final) + final)
        ahead = (1 - turn) * (1 - final) * (x_hi - x_lo + (it == last - 2).astype(jnp.int32))
        lax.fori_loop(x_lo, x_lo + ahead, spread, 0)
        lax.fori_loop(x_lo, x_hi, stage_x, 0)
        c_lo = it * (1 - final) + (n - 1) * final
        lax.fori_loop(c_lo, c_lo + 2 * turn + (it == 0).astype(jnp.int32) + final, stage_c, 0)
        return 0

    lax.fori_loop(0, last + 1, event, 0)

    def up_tile(i, _):
        col = pl.ds(pl.multiple_of(i * 256, 256), 256)
        res = dot(xc[0, :, col], grd[...], TN)
        for e in range(local):
            gup_ref[e, col, :] = res[:, e * ff : (e + 1) * ff].astype(BF16)
        return 0

    def down_tile(i, _):
        col = pl.ds(pl.multiple_of(i * 256, 256), 256)
        gdn_ref[col, :] = dot(hid[:, col], xc[1], TN).astype(BF16)
        return 0

    n_up, n_down = width // 256, lff // 256

    def fill_up(lo, hi):
        lax.fori_loop(lo, hi, up_tile, 0)

    def fill_down(lo, hi):
        lax.fori_loop(lo, hi, down_tile, 0)

    sib_part(half)
    for t in range(half):
        send_sum(t, 0, t == 0)
        if t == 1:
            fill_down(0, 1)
        if t + 2 < half:
            early(t + 2)
        if t == 0:
            fill_up(0, n_up // 2)
        elif t == 1:
            fill_up(n_up // 2, n_up)
        elif t == 2:
            fill_down(1, 2)
    pass_on(1)
    fill_down(2 if half > 2 else 1, n_down)
    pass_on(0)
    own_part.wait_recv()
    for side_of in (1, 0):
        for d, c in quarters_of(side_of):
            hop(d, half, c).wait_recv()
            got = rsr[d, half - 1, :, quarters[c]].astype(F32)
            if side_of == 1:
                own[0, :, quarters[c]] = finr[:, quarters[c]].astype(F32) + got
            else:
                out_ref[:, quarters[c]] = (own[0, :, quarters[c]] + got).astype(BF16)

    for h in (0, 1):
        cot_in(h).wait_send()
    own_part.wait_send()
    for d in (0, 1):
        for s in range(1, half):
            ring(xc.at[0, rows(me)], me, d, s).wait_send()
        ring_last(me, d).wait_send()
        for s in range(half):
            owner = a - s + 2 * s * d

            @pl.when(reaches(d) & (owner >= 0) & (owner < half))
            def _():
                for h in (0, 1):
                    column(owner, s, d, h).wait_send()

    for owner in range(half):
        for h in (0, 1):
            row(owner, h).wait_send()
    for r in range(n):
        side(xc.at[0, rows(me)], r, me).wait_send()
        for h in (0, 1):
            cot_side(r, h).wait_send()
        remote(sibsend.at[r], sibrecv.at[r], ps_s.at[r], ps_r.at[r], here(sib)).wait_send()

    def told(i, _):
        to = lax.rem(me + i, ep)
        remote(idt_ref, idt.at[me], id_s.at[i], id_r.at[me], here(to)).wait_send()
        remote(paysend.at[to], pay.at[me], pay_s.at[i], pay_r.at[me], here(to)).wait_send()
        return 0

    lax.fori_loop(1, ep, told, 0)
    for d in (0, 1):
        for t in range(half):
            for c in range(4):
                if t > 0 or c // 2 == d:
                    hop(d, t + 1, c).wait_send()
        for c in range(4):
            cross(d, c).wait_send()


def put_out(*refs):
    ins, outs, sems = refs[:3], refs[3:6], refs[6]
    copies = [pltpu.make_async_copy(src, dst, sems.at[i]) for i, (src, dst) in enumerate(zip(ins, outs))]
    for c in copies:
        c.start()
    for c in copies:
        c.wait()


def fused_body(ns, ep, inputs, upstream, gate_saved, expert_ids, route_weights, w_up, w_down):
    toks, top = expert_ids.shape[1:]
    local, width, ff = w_up.shape[1:]
    experts = local * ep
    cap = 3 * toks * top // (2 * experts)
    n, half = ep // 2, ep // 4
    lff, lcap = local * ff, local * cap
    flat = toks * top
    hbm = pl.BlockSpec(memory_space=pl.ANY)
    vmem = pl.BlockSpec(memory_space=pltpu.VMEM)
    dma = pltpu.SemaphoreType.DMA
    out, gup, gdn = pl.pallas_call(
        functools.partial(kernel, ns, ep, toks, top, width, ff, local, cap),
        out_shape=(
            pltpu.VMEM((toks, width), BF16),
            pltpu.VMEM((local, width, ff), BF16),
            pltpu.VMEM((lff, width), BF16),
        ),
        in_specs=[hbm] * 5 + [vmem] * 2,
        out_specs=(vmem, vmem, vmem),
        scratch_shapes=[
            pltpu.VMEM((2, ep * toks, width), BF16),
            pltpu.VMEM((ep, lcap, ff), BF16),
            pltpu.VMEM((ep, lcap, ff), BF16),
            pltpu.VMEM((ep, top, toks), jnp.int32),
            pltpu.VMEM((flat, ff), BF16),
            pltpu.VMEM((flat, ff), BF16),
            pltpu.VMEM((flat // 256, 256), F32),
            pltpu.VMEM((flat // 256, 256), F32),
            pltpu.VMEM((width, lff), BF16),
            pltpu.VMEM((lff, width), BF16),
            pltpu.VMEM((ep * toks, lff), BF16),
            pltpu.VMEM((ep * toks, lff), BF16),
            pltpu.VMEM((2 * toks, width), F32),
            pltpu.VMEM((n, toks, width), F32),
            pltpu.VMEM((n, toks, width), BF16),
            pltpu.VMEM((n, toks, width), BF16),
            pltpu.VMEM((2, half, toks, width), BF16),
            pltpu.VMEM((2, half, toks, width), BF16),
            pltpu.VMEM((toks, width), BF16),
            pltpu.VMEM((toks, width), BF16),
            pltpu.VMEM((2, toks, width), BF16),
            dma((2 * (half + 1),)),
            dma((2 * (half + 1),)),
            dma((4 * half,)),
            dma((2 * half,)),
            dma((2 * n,)),
            dma((3 * n,)),
            dma((3 * n,)),
            dma((ep,)),
            dma((ep,)),
            dma((ep,)),
            dma((ep,)),
            dma((n,)),
            dma((n,)),
            dma((8 * (half + 1),)),
            dma((8 * (half + 1),)),
            dma((3,)),
            dma((3,)),
            dma((8,)),
            dma((8,)),
            dma((3 + local,)),
        ],
        compiler_params=pltpu.CompilerParams(
            collective_id=0, has_side_effects=True, vmem_limit_bytes=VMEM_BYTES
        ),
    )(
        inputs[0], upstream[0], gate_saved[0].reshape(flat, ff), w_up[0],
        w_down[0].reshape(lff, width), expert_ids[0].T, route_weights[0].T,
    )
    res = tuple(pltpu.with_memory_space_constraint(r, pltpu.VMEM) for r in (out, gup, gdn))
    out, gup, gdn = pl.pallas_call(
        put_out,
        out_shape=tuple(pltpu.HBM(r.shape, r.dtype) for r in res),
        in_specs=[vmem] * 3,
        out_specs=(hbm, hbm, hbm),
        scratch_shapes=[dma((3,))],
        compiler_params=pltpu.CompilerParams(vmem_limit_bytes=2**22),
    )(*res)
    return out[None], gup[None], gdn.reshape(1, local, ff, width)


def from_behind(block, axis, distance):
    devices = range(lax.axis_size(axis))
    route = [((i - distance) % len(devices), i) for i in devices]
    return lax.ppermute(block, axis, route)


def plain_body(inputs, upstream, gate_saved, expert_ids, route_weights, w_up, w_down):
    ep = lax.axis_size("ep")
    local = w_up.shape[1]
    experts = local * ep
    toks, top = expert_ids.shape[1:]
    cap = 3 * toks * top // (2 * experts)
    width = inputs.shape[2]
    ff = w_up.shape[3]

    routing = jnp.concatenate([expert_ids[0].astype(F32), route_weights[0]], axis=1)
    routing_all = lax.all_gather(routing, "ep", axis=0, tiled=False)

    ids = expert_ids[0]
    hit = ids[:, :, None] == jnp.arange(experts, dtype=jnp.int32)
    member = jnp.any(hit, axis=1).astype(BF16)
    lower = (jnp.arange(toks)[:, None] > jnp.arange(toks)[None, :]).astype(BF16)
    rank = jnp.dot(lower, member, preferred_element_type=F32)
    place = jnp.sum(jnp.where(hit, rank[:, None, :], 0.0), axis=2)
    slot = (ids * cap + place.astype(jnp.int32)).reshape(1, toks * top)
    pick = (jnp.arange(experts * cap, dtype=jnp.int32)[:, None] == slot).astype(BF16)
    gate_send = jnp.dot(pick, gate_saved[0].reshape(toks * top, ff), preferred_element_type=F32)
    gate_send = gate_send.astype(BF16).reshape(ep, local, cap, ff)
    gate_recv = lax.all_to_all(gate_send, "ep", split_axis=0, concat_axis=0, tiled=True)

    cot = from_behind(upstream, "section", -1)[0]
    x_all = lax.all_gather(inputs[0], "ep", axis=0, tiled=True)
    c_all = lax.all_gather(cot, "ep", axis=0, tiled=True)

    me = lax.axis_index("ep")
    mine = (me * local + jnp.arange(local)).astype(F32)
    hits = routing_all[:, :, :top, None] == mine
    weight = jnp.sum(jnp.where(hits, routing_all[:, :, top:, None], 0.0), axis=2)
    members = jnp.any(hits, axis=2)
    ranks = jnp.einsum("ab,sbe->sae", lower, members.astype(BF16), preferred_element_type=F32)
    ranks = jnp.where(members, ranks, -1.0)
    spread = (ranks[:, :, :, None] == jnp.arange(cap).astype(F32)).astype(BF16)
    gate = jnp.einsum("stec,secf->stef", spread, gate_recv, preferred_element_type=F32)
    act = jax.nn.silu(gate).reshape(ep * toks, local, ff)
    act_w = (act * weight.reshape(ep * toks, local, 1)).reshape(ep * toks, local * ff)

    up_cat = jnp.transpose(w_up[0], (1, 0, 2)).reshape(width, local * ff)
    down_cat = w_down[0].reshape(local * ff, width)
    u = jnp.dot(x_all, up_cat, preferred_element_type=F32)
    hidden = (act_w * u).astype(BF16)
    h = dot(c_all, down_cat, NT)
    g = (act_w * h).astype(BF16)
    part = dot(g, up_cat, NT)
    grad = lax.psum_scatter(part.astype(BF16), "ep", scatter_dimension=0, tiled=True)
    delivered = from_behind(grad[None], "section", -1)
    grad_down = dot(hidden, c_all, TN)
    grad_up = jnp.stack([dot(x_all, g[:, e * ff : (e + 1) * ff], TN) for e in range(local)])
    return (
        delivered,
        grad_up.astype(BF16)[None],
        grad_down.astype(BF16).reshape(1, local, ff, width),
    )


def solution(mesh):
    ns, ep = mesh.shape["section"], mesh.shape["ep"]

    def body(*args):
        toks, width = args[0].shape[1:]
        local, ff = args[5].shape[1], args[5].shape[3]
        rows = ep * toks
        need = rows * (4 * width + 4 * local * ff) + 12 * rows * width // 2 + 4 * local * ff * width
        if need < 0.75 * VMEM_BYTES and ep % 8 == 0:
            return fused_body(ns, ep, *args)
        return plain_body(*args)

    return jax.shard_map(
        body,
        mesh=mesh,
        in_specs=(
            P("section", "ep", None),
            P("section", "ep", None),
            P("section", "ep", None, None),
            P("section", "ep", None),
            P("section", "ep", None),
            P("section", "ep", None, None),
            P("section", "ep", None, None),
        ),
        out_specs=(
            P("section", "ep", None),
            P("section", "ep", None, None),
            P("section", "ep", None, None),
        ),
        check_vma=False,
    )
```

```python
import functools

import jax
import jax.numpy as jnp
from jax import lax
from jax.experimental import pallas as pl
from jax.experimental.pallas import tpu as pltpu
from jax.sharding import PartitionSpec as P

BF16 = jnp.bfloat16
F32 = jnp.float32
MESH = pl.DeviceIdType.MESH
VMEM_BYTES = 58_000_000
TN = (((0,), (0,)), ((), ()))
NT = (((1,), (1,)), ((), ()))


def dot(a, b, dims=(((1,), (0,)), ((), ()))):
    return lax.dot_general(a, b, dims, preferred_element_type=F32)


def iota(shape, dim):
    return lax.broadcasted_iota(jnp.int32, shape, dim)


def kernel(
    ns, ep, toks, top, width, ff, local, cap,
    x_in, up_in, gate_in, wup_in, wdn_in, idt_ref, wt_ref,
    out_ref, gup_ref, gdn_ref,
    xc, pay, paysend, idt, gate, act, slots, wflat, wup, wdn, hid, grd,
    own, sibsend, sibrecv, rss, rsr, fin, finr, over,
    ring_s, ring_r, col_s, row_s, cot_r, sib_s, sib_r, pay_s, pay_r, id_s, id_r, ps_s, ps_r, rs_s, rs_r,
    y_s, y_r, over_s, over_r, loc,
):
    n = ep // 2
    half = n // 2
    sec = lax.axis_index("section")
    me = lax.axis_index("ep")
    core = lax.rem(me, 2)
    chip = lax.div(me, 2)
    sib = me + 1 - 2 * core
    a, b = lax.div(chip, 2), lax.rem(chip, 2)
    pos = (1 - b) * a + b * (n - 1 - a)
    w2, w4 = width // 2, width // 4
    cols = [slice(0, w2), slice(w2, width)]
    quarters = [slice(c * w4, (c + 1) * w4) for c in range(4)]
    lff = local * ff
    lcap = local * cap
    two = 2 * toks

    def chip_at(q):
        h = lax.div(q, half)
        return (1 - h) * (2 * q) + h * (2 * (n - 1 - q) + 1)

    def rows(dev):
        return pl.ds(pl.multiple_of(dev * toks, toks), toks)

    def here(dev):
        return (sec, dev)

    def remote(src, dst, s, r, to):
        return pltpu.make_async_remote_copy(
            src_ref=src, dst_ref=dst, send_sem=s, recv_sem=r, device_id=to, device_id_type=MESH
        )

    nxt = [chip_at(lax.rem(pos + 1, n)) * 2 + core, chip_at(lax.rem(pos + n - 1, n)) * 2 + core]
    sec_to = lax.rem(sec + ns - 1, ns)
    sec_from = lax.rem(sec + 1, ns)

    bar = pltpu.get_barrier_semaphore()
    across = [me]
    greet = [(sec_to, dev) for dev in across] + ([(sec_from, dev) for dev in across] if ns > 2 else [])

    def hello(i, _):
        pl.semaphore_signal(bar, inc=1, device_id=here(lax.rem(me + i, ep)), device_id_type=MESH)
        return 0

    for to in greet:
        pl.semaphore_signal(bar, inc=1, device_id=to, device_id_type=MESH)
    lax.fori_loop(1, ep, hello, 0)

    local_copies = [
        pltpu.make_async_copy(x_in, xc.at[0, rows(me)], loc.at[0]),
        pltpu.make_async_copy(gate_in, gate, loc.at[1]),
        pltpu.make_async_copy(wdn_in, wdn, loc.at[2]),
    ] + [
        pltpu.make_async_copy(wup_in.at[e], wup.at[:, pl.ds(e * ff, ff)], loc.at[3 + e]) for e in range(local)
    ]
    for c in local_copies:
        c.start()
    pl.semaphore_wait(bar, ep - 1 + len(greet))

    def ring(src, dev, d, s):
        i = d * (half + 1) + s
        return remote(src, xc.at[0, rows(dev)], ring_s.at[i], ring_r.at[i], here(nxt[d]))

    def ring_last(dev, d):
        ref = xc.at[0, rows(dev), cols[d]]
        i = d * (half + 1) + half
        return remote(ref, ref, ring_s.at[i], ring_r.at[i], here(nxt[d]))

    def side(src, q, dev):
        return remote(src, xc.at[0, rows(dev)], sib_s.at[q * 3], sib_r.at[q * 3], here(sib))

    def cot_ref(q, h, of=core):
        return xc.at[1, rows(q * 2 + of), cols[h]]

    def column(owner, s, d, h):
        ref = cot_ref(owner * 2 + b, h)
        to = ((a + 1 - 2 * d) * 2 + b) * 2 + core
        return remote(
            ref, ref, col_s.at[(d * half + s) * 2 + h], cot_r.at[(owner * 2 + b) * 2 + h], here(to)
        )

    def row(owner, h):
        ref = cot_ref(owner * 2 + b, h)
        to = (a * 2 + 1 - b) * 2 + core
        return remote(ref, ref, row_s.at[owner * 2 + h], cot_r.at[(owner * 2 + b) * 2 + h], here(to))

    def cot_arrive(q, h):
        ref = cot_ref(q, h)
        remote(ref, ref, row_s.at[h], cot_r.at[q * 2 + h], here(sib)).wait_recv()

    def cot_side(q, h, of=core):
        ref = cot_ref(q, h, of)
        return remote(ref, ref, sib_s.at[q * 3 + 1 + h], sib_r.at[q * 3 + 1 + h], here(sib))

    def cot_in(h):
        return remote(up_in.at[:, cols[h]], cot_ref(chip, h), y_s.at[h], y_r.at[h], (sec_to, me))

    for h in (0, 1):
        cot_in(h).start()
    for d in (0, 1):
        ring(x_in, me, d, 1).start()
    side(x_in, chip, me).start()
    idt[me] = idt_ref[...]

    def tell(i, _):
        to = lax.rem(me + i, ep)
        remote(idt_ref, idt.at[me], id_s.at[i], id_r.at[me], here(to)).start()
        return 0

    lax.fori_loop(1, ep, tell, 0)

    experts = ep * local
    lanes = 256
    parts = toks * top // lanes
    span = lanes // top
    tri = (iota((lanes, lanes), 0) < iota((lanes, lanes), 1)).astype(BF16)
    base = jnp.zeros((experts, 1), F32)
    ids_t = idt_ref[...].astype(F32).astype(BF16)
    w_t = wt_ref[...].astype(BF16)
    mine_k = iota((top, lanes), 0) == lax.rem(iota((top, lanes), 1), top)
    for k in range(parts):
        token = lax.div(iota((toks, lanes), 1), top) + k * span
        take = (iota((toks, lanes), 0) == token).astype(BF16)
        ids = jnp.sum(jnp.where(mine_k, dot(ids_t, take), 0.0), axis=0, keepdims=True)
        wflat[k : k + 1, :] = jnp.sum(jnp.where(mine_k, dot(w_t, take), 0.0), axis=0, keepdims=True)
        hot = (iota((experts, lanes), 0).astype(F32) == ids).astype(F32)
        cum = dot(hot.astype(BF16), tri) + base
        base = base + jnp.sum(hot, axis=1, keepdims=True)
        slots[k : k + 1, :] = ids * cap + jnp.sum(hot * cum, axis=0, keepdims=True)

    local_copies[1].wait()

    def silu_rows(k, _):
        r = pl.ds(pl.multiple_of(k * lanes, lanes), lanes)
        v = gate[r, :].astype(F32)
        act[r, :] = (v / (1.0 + jnp.exp(-v))).astype(BF16)
        return 0

    lax.fori_loop(0, parts, silu_rows, 0)
    group = 4 * lcap

    def pack(m, _):
        acc = jnp.zeros((group, ff), F32)
        at = (iota((group, lanes), 0) + m * group).astype(F32)
        for k in range(parts):
            pick = jnp.where(at == slots[k : k + 1, :], wflat[k : k + 1, :], 0.0).astype(BF16)
            acc = acc + dot(pick, act[k * lanes : (k + 1) * lanes, :])
        for j in range(4):
            paysend[m * 4 + j] = acc[j * lcap : (j + 1) * lcap].astype(BF16)
        return 0

    lax.fori_loop(0, ep // 4, pack, 0)

    def give(i, _):
        to = lax.rem(me + i, ep)
        remote(paysend.at[to], pay.at[me], pay_s.at[i], pay_r.at[me], here(to)).start()
        return 0

    lax.fori_loop(1, ep, give, 0)
    pay[me] = paysend[me]

    def reaches(d):
        return (a + 1 < half) if d == 0 else (a >= 1)

    for h in (0, 1):
        cot_in(h).wait_recv()
        for d in (0, 1):

            @pl.when(reaches(d))
            def _():
                column(a, 0, d, h).start()

        row(a, h).start()
        cot_side(chip, h).start()
    for c in [local_copies[0]] + local_copies[2:]:
        c.wait()

    upper = (iota((toks, toks), 0) < iota((toks, toks), 1)).astype(BF16)

    def chunk_of(k):
        odd = lax.rem(k, 2)
        r = odd * lax.div(k + 1, 2) + (1 - odd) * lax.rem(n - lax.div(k, 2), n)
        q = chip_at(lax.rem(pos + r, n))
        return r, q, pl.ds(pl.multiple_of(q * two, two), two)

    def spread(k, _):
        r, q, both = chunk_of(k)
        for j in (0, 1):
            src = q * 2 + j

            @pl.when(src != me)
            def _():
                remote(paysend.at[src], pay.at[src], pay_s.at[0], pay_r.at[src], here(src)).wait_recv()
                remote(idt_ref, idt.at[src], id_s.at[0], id_r.at[src], here(src)).wait_recv()

            names = idt[src]
            for e in range(local):
                member = jnp.sum((names == me * local + e).astype(F32), axis=0, keepdims=True)
                rank = dot(jnp.broadcast_to(member, (8, toks)).astype(BF16), upper)[0:1, :]
                key = jnp.where(member > 0.0, rank, -1.0)
                to_slot = (iota((cap, toks), 0).astype(F32) == key).astype(BF16)
                grd[rows(src), e * ff : (e + 1) * ff] = dot(
                    to_slot, pay[src, e * cap : (e + 1) * cap, :], TN
                ).astype(BF16)
        return 0

    def stage_x(k, _):
        r, q, both = chunk_of(k)
        dev = q * 2 + 1 - core
        side(xc.at[0, rows(dev)], q, dev).wait_recv()
        hid[both, :] = (grd[both, :].astype(F32) * dot(xc[0, both, :], wup[...])).astype(BF16)
        return 0

    def stage_c(k, _):
        r, q, both = chunk_of(k)
        for h in (0, 1):
            cot_side(q, h, 1 - core).wait_recv()
        g = (grd[both, :].astype(F32) * dot(xc[1, both, :], wdn[...], NT)).astype(BF16)
        grd[both, :] = g
        sibsend[r] = dot(grd[rows(q * 2 + 1 - core), :], wup[...], NT).astype(BF16)
        remote(sibsend.at[r], sibrecv.at[r], ps_s.at[r], ps_r.at[r], here(sib)).start()
        own[r] = dot(grd[rows(q * 2 + core), :], wup[...], NT)
        return 0

    def hop(d, t, c):
        i = (d * (half + 1) + t) * 4 + c
        ref = quarters[c]
        src = over.at[d, :, ref] if t == half else rss.at[d, t - 1, :, ref]
        return remote(src, rsr.at[d, t - 1, :, ref], rs_s.at[i], rs_r.at[i], here(nxt[d]))

    def cross(d, c):
        i = d * 4 + c
        ref = quarters[c]
        return remote(rss.at[d, half - 1, :, ref], over.at[d, :, ref], over_s.at[i], over_r.at[i], (sec_to, me))

    def quarters_of(side_of):
        return [(d, 2 * (d if side_of == 0 else 1 - d) + j) for j in (0, 1) for d in (0, 1)]

    def pass_on(side_of):
        for d, c in quarters_of(side_of):
            cross(d, c).wait_recv()
            hop(d, half, c).start()

    def sib_part(r):
        remote(sibsend.at[r], sibrecv.at[r], ps_s.at[r], ps_r.at[r], here(sib)).wait_recv()

    def send_sum(t, side_of, first, ways=(0, 1)):
        for d, c in [p for p in quarters_of(side_of) if p[0] in ways]:
            r = (half - t) if d == 0 else n - (half - t)
            total = own[r, :, quarters[c]] + sibrecv[r, :, quarters[c]].astype(F32)
            if not first:
                hop(d, t, c).wait_recv()
                total = total + rsr[d, t - 1, :, quarters[c]].astype(F32)
            rss[d, t, :, quarters[c]] = total.astype(BF16)
            if t + 1 < half:
                hop(d, t + 1, c).start()
            else:
                cross(d, c).start()

    def early(t):
        for d in (0, 1):
            sib_part((half - t) if d == 0 else n - (half - t))
            if t == 1:
                send_sum(t, 1, True, (d,))
        if t > 1:
            send_sum(t, 1, False)

    own_part = remote(fin, finr, y_s.at[2], y_r.at[2], (sec_to, me))

    last = 2 * half - 2

    def event(it, _):
        s = lax.div(it, 2) + 1
        turn = lax.rem(it, 2)

        @pl.when((it < last) & (turn == 0))
        def _():
            for d in (0, 1):
                q = chip_at(lax.rem(pos + ((n - s) if d == 0 else s), n))
                dev = q * 2 + core
                src = xc.at[0, rows(dev)]
                ring(src, dev, d, s).wait_recv()

                @pl.when(s + 1 < half)
                def _():
                    ring(src, dev, d, s + 1).start()

                @pl.when(s + 1 == half)
                def _():
                    ring_last(dev, d).start()

                side(src, q, dev).start()

        def from_row(owner):
            @pl.when((owner >= 0) & (owner < half))
            def _():
                q = owner * 2 + 1 - b
                for h in (0, 1):
                    cot_arrive(q, h)
                    cot_side(q, h).start()

        @pl.when((it < last) & (turn == 1))
        def _():
            for h in (0, 1):
                for d in (0, 1):
                    owner = a - s + 2 * s * d

                    @pl.when((owner >= 0) & (owner < half))
                    def _():
                        q = owner * 2 + b
                        cot_arrive(q, h)

                        @pl.when(reaches(d))
                        def _():
                            column(owner, s, d, h).start()

                        row(owner, h).start()
                        cot_side(q, h).start()

            from_row(a + s - 1)

            @pl.when(s > 1)
            def _():
                from_row(a - s + 1)

        @pl.when(it == 2)
        def _():
            sib_part(0)
            fin[...] = (own[0] + sibrecv[0].astype(F32)).astype(BF16)
            own_part.start()

        @pl.when(it == last)
        def _():
            q = chip_at(lax.rem(pos + half, n))
            dev = q * 2 + core
            for d in (0, 1):
                ring_last(dev, d).wait_recv()
            side(xc.at[0, rows(dev)], q, dev).start()
            early(1)
            from_row(a + half - 1)
            from_row(a - half + 1)

        final = (it == last).astype(jnp.int32)
        x_lo = (it + jnp.minimum(it, 1)) * (1 - final) + (n - 1) * final
        x_hi = x_lo + (1 - turn) * ((2 + (it == 0).astype(jnp.int32)) * (1 - final) + final)
        ahead = (1 - turn) * (1 - final) * (x_hi - x_lo + (it == last - 2).astype(jnp.int32))
        lax.fori_loop(x_lo, x_lo + ahead, spread, 0)
        lax.fori_loop(x_lo, x_hi, stage_x, 0)
        c_lo = it * (1 - final) + (n - 1) * final
        lax.fori_loop(c_lo, c_lo + 2 * turn + (it == 0).astype(jnp.int32) + final, stage_c, 0)
        return 0

    lax.fori_loop(0, last + 1, event, 0)

    def up_tile(i, _):
        col = pl.ds(pl.multiple_of(i * 256, 256), 256)
        res = dot(xc[0, :, col], grd[...], TN)
        for e in range(local):
            gup_ref[e, col, :] = res[:, e * ff : (e + 1) * ff].astype(BF16)
        return 0

    def down_tile(i, _):
        col = pl.ds(pl.multiple_of(i * 256, 256), 256)
        gdn_ref[col, :] = dot(hid[:, col], xc[1], TN).astype(BF16)
        return 0

    n_up, n_down = width // 256, lff // 256

    def fill_up(lo, hi):
        lax.fori_loop(lo, hi, up_tile, 0)

    def fill_down(lo, hi):
        lax.fori_loop(lo, hi, down_tile, 0)

    sib_part(half)
    for t in range(half):
        send_sum(t, 0, t == 0)
        if t == 1:
            fill_down(0, 1)
        if t + 2 < half:
            early(t + 2)
        if t == 0:
            fill_up(0, n_up // 2)
        elif t == 1:
            fill_up(n_up // 2, n_up)
        elif t == 2:
            fill_down(1, 2)
    pass_on(1)
    fill_down(2 if half > 2 else 1, n_down)
    pass_on(0)
    own_part.wait_recv()
    for side_of in (1, 0):
        for d, c in quarters_of(side_of):
            hop(d, half, c).wait_recv()
            got = rsr[d, half - 1, :, quarters[c]].astype(F32)
            if side_of == 1:
                own[0, :, quarters[c]] = finr[:, quarters[c]].astype(F32) + got
            else:
                out_ref[:, quarters[c]] = (own[0, :, quarters[c]] + got).astype(BF16)

    for h in (0, 1):
        cot_in(h).wait_send()
    own_part.wait_send()
    for d in (0, 1):
        for s in range(1, half):
            ring(xc.at[0, rows(me)], me, d, s).wait_send()
        ring_last(me, d).wait_send()
        for s in range(half):
            owner = a - s + 2 * s * d

            @pl.when(reaches(d) & (owner >= 0) & (owner < half))
            def _():
                for h in (0, 1):
                    column(owner, s, d, h).wait_send()

    for owner in range(half):
        for h in (0, 1):
            row(owner, h).wait_send()
    for r in range(n):
        side(xc.at[0, rows(me)], r, me).wait_send()
        for h in (0, 1):
            cot_side(r, h).wait_send()
        remote(sibsend.at[r], sibrecv.at[r], ps_s.at[r], ps_r.at[r], here(sib)).wait_send()

    def told(i, _):
        to = lax.rem(me + i, ep)
        remote(idt_ref, idt.at[me], id_s.at[i], id_r.at[me], here(to)).wait_send()
        remote(paysend.at[to], pay.at[me], pay_s.at[i], pay_r.at[me], here(to)).wait_send()
        return 0

    lax.fori_loop(1, ep, told, 0)
    for d in (0, 1):
        for t in range(half):
            for c in range(4):
                if t > 0 or c // 2 == d:
                    hop(d, t + 1, c).wait_send()
        for c in range(4):
            cross(d, c).wait_send()


def put_out(*refs):
    ins, outs, sems = refs[:3], refs[3:6], refs[6]
    copies = [pltpu.make_async_copy(src, dst, sems.at[i]) for i, (src, dst) in enumerate(zip(ins, outs))]
    for c in copies:
        c.start()
    for c in copies:
        c.wait()


def fused_body(ns, ep, inputs, upstream, gate_saved, expert_ids, route_weights, w_up, w_down):
    toks, top = expert_ids.shape[1:]
    local, width, ff = w_up.shape[1:]
    experts = local * ep
    cap = 3 * toks * top // (2 * experts)
    n, half = ep // 2, ep // 4
    lff, lcap = local * ff, local * cap
    flat = toks * top
    hbm = pl.BlockSpec(memory_space=pl.ANY)
    vmem = pl.BlockSpec(memory_space=pltpu.VMEM)
    dma = pltpu.SemaphoreType.DMA
    out, gup, gdn = pl.pallas_call(
        functools.partial(kernel, ns, ep, toks, top, width, ff, local, cap),
        out_shape=(
            pltpu.VMEM((toks, width), BF16),
            pltpu.VMEM((local, width, ff), BF16),
            pltpu.VMEM((lff, width), BF16),
        ),
        in_specs=[hbm] * 5 + [vmem] * 2,
        out_specs=(vmem, vmem, vmem),
        scratch_shapes=[
            pltpu.VMEM((2, ep * toks, width), BF16),
            pltpu.VMEM((ep, lcap, ff), BF16),
            pltpu.VMEM((ep, lcap, ff), BF16),
            pltpu.VMEM((ep, top, toks), jnp.int32),
            pltpu.VMEM((flat, ff), BF16),
            pltpu.VMEM((flat, ff), BF16),
            pltpu.VMEM((flat // 256, 256), F32),
            pltpu.VMEM((flat // 256, 256), F32),
            pltpu.VMEM((width, lff), BF16),
            pltpu.VMEM((lff, width), BF16),
            pltpu.VMEM((ep * toks, lff), BF16),
            pltpu.VMEM((ep * toks, lff), BF16),
            pltpu.VMEM((n, toks, width), F32),
            pltpu.VMEM((n, toks, width), BF16),
            pltpu.VMEM((n, toks, width), BF16),
            pltpu.VMEM((2, half, toks, width), BF16),
            pltpu.VMEM((2, half, toks, width), BF16),
            pltpu.VMEM((toks, width), BF16),
            pltpu.VMEM((toks, width), BF16),
            pltpu.VMEM((2, toks, width), BF16),
            dma((2 * (half + 1),)),
            dma((2 * (half + 1),)),
            dma((4 * half,)),
            dma((2 * half,)),
            dma((2 * n,)),
            dma((3 * n,)),
            dma((3 * n,)),
            dma((ep,)),
            dma((ep,)),
            dma((ep,)),
            dma((ep,)),
            dma((n,)),
            dma((n,)),
            dma((8 * (half + 1),)),
            dma((8 * (half + 1),)),
            dma((3,)),
            dma((3,)),
            dma((8,)),
            dma((8,)),
            dma((3 + local,)),
        ],
        compiler_params=pltpu.CompilerParams(
            collective_id=0, has_side_effects=True, vmem_limit_bytes=VMEM_BYTES
        ),
    )(
        inputs[0], upstream[0], gate_saved[0].reshape(flat, ff), w_up[0],
        w_down[0].reshape(lff, width), expert_ids[0].T, route_weights[0].T,
    )
    res = tuple(pltpu.with_memory_space_constraint(r, pltpu.VMEM) for r in (out, gup, gdn))
    out, gup, gdn = pl.pallas_call(
        put_out,
        out_shape=tuple(pltpu.HBM(r.shape, r.dtype) for r in res),
        in_specs=[vmem] * 3,
        out_specs=(hbm, hbm, hbm),
        scratch_shapes=[dma((3,))],
        compiler_params=pltpu.CompilerParams(vmem_limit_bytes=2**22),
    )(*res)
    return out[None], gup[None], gdn.reshape(1, local, ff, width)


def from_behind(block, axis, distance):
    devices = range(lax.axis_size(axis))
    route = [((i - distance) % len(devices), i) for i in devices]
    return lax.ppermute(block, axis, route)


def plain_body(inputs, upstream, gate_saved, expert_ids, route_weights, w_up, w_down):
    ep = lax.axis_size("ep")
    local = w_up.shape[1]
    experts = local * ep
    toks, top = expert_ids.shape[1:]
    cap = 3 * toks * top // (2 * experts)
    width = inputs.shape[2]
    ff = w_up.shape[3]

    routing = jnp.concatenate([expert_ids[0].astype(F32), route_weights[0]], axis=1)
    routing_all = lax.all_gather(routing, "ep", axis=0, tiled=False)

    ids = expert_ids[0]
    hit = ids[:, :, None] == jnp.arange(experts, dtype=jnp.int32)
    member = jnp.any(hit, axis=1).astype(BF16)
    lower = (jnp.arange(toks)[:, None] > jnp.arange(toks)[None, :]).astype(BF16)
    rank = jnp.dot(lower, member, preferred_element_type=F32)
    place = jnp.sum(jnp.where(hit, rank[:, None, :], 0.0), axis=2)
    slot = (ids * cap + place.astype(jnp.int32)).reshape(1, toks * top)
    pick = (jnp.arange(experts * cap, dtype=jnp.int32)[:, None] == slot).astype(BF16)
    gate_send = jnp.dot(pick, gate_saved[0].reshape(toks * top, ff), preferred_element_type=F32)
    gate_send = gate_send.astype(BF16).reshape(ep, local, cap, ff)
    gate_recv = lax.all_to_all(gate_send, "ep", split_axis=0, concat_axis=0, tiled=True)

    cot = from_behind(upstream, "section", -1)[0]
    x_all = lax.all_gather(inputs[0], "ep", axis=0, tiled=True)
    c_all = lax.all_gather(cot, "ep", axis=0, tiled=True)

    me = lax.axis_index("ep")
    mine = (me * local + jnp.arange(local)).astype(F32)
    hits = routing_all[:, :, :top, None] == mine
    weight = jnp.sum(jnp.where(hits, routing_all[:, :, top:, None], 0.0), axis=2)
    members = jnp.any(hits, axis=2)
    ranks = jnp.einsum("ab,sbe->sae", lower, members.astype(BF16), preferred_element_type=F32)
    ranks = jnp.where(members, ranks, -1.0)
    spread = (ranks[:, :, :, None] == jnp.arange(cap).astype(F32)).astype(BF16)
    gate = jnp.einsum("stec,secf->stef", spread, gate_recv, preferred_element_type=F32)
    act = jax.nn.silu(gate).reshape(ep * toks, local, ff)
    act_w = (act * weight.reshape(ep * toks, local, 1)).reshape(ep * toks, local * ff)

    up_cat = jnp.transpose(w_up[0], (1, 0, 2)).reshape(width, local * ff)
    down_cat = w_down[0].reshape(local * ff, width)
    u = jnp.dot(x_all, up_cat, preferred_element_type=F32)
    hidden = (act_w * u).astype(BF16)
    h = dot(c_all, down_cat, NT)
    g = (act_w * h).astype(BF16)
    part = dot(g, up_cat, NT)
    grad = lax.psum_scatter(part.astype(BF16), "ep", scatter_dimension=0, tiled=True)
    delivered = from_behind(grad[None], "section", -1)
    grad_down = dot(hidden, c_all, TN)
    grad_up = jnp.stack([dot(x_all, g[:, e * ff : (e + 1) * ff], TN) for e in range(local)])
    return (
        delivered,
        grad_up.astype(BF16)[None],
        grad_down.astype(BF16).reshape(1, local, ff, width),
    )


def solution(mesh):
    ns, ep = mesh.shape["section"], mesh.shape["ep"]

    def body(*args):
        toks, width = args[0].shape[1:]
        local, ff = args[5].shape[1], args[5].shape[3]
        rows = ep * toks
        need = rows * (4 * width + 4 * local * ff) + 12 * rows * width // 2 + 4 * local * ff * width
        if need < 0.75 * VMEM_BYTES and ep % 8 == 0:
            return fused_body(ns, ep, *args)
        return plain_body(*args)

    return jax.shard_map(
        body,
        mesh=mesh,
        in_specs=(
            P("section", "ep", None),
            P("section", "ep", None),
            P("section", "ep", None, None),
            P("section", "ep", None),
            P("section", "ep", None),
            P("section", "ep", None, None),
            P("section", "ep", None, None),
        ),
        out_specs=(
            P("section", "ep", None),
            P("section", "ep", None, None),
            P("section", "ep", None, None),
        ),
        check_vma=False,
    )
```
